8 devices in a mesh: dp: 1 (over z), tp: 2 (over y), cp: 4 (over x, core).
Axes of the slice: x: 2, y: 2, z: 1, core: 2. Of those that a mesh axis runs over, the one named last changes fastest.
Arguments:
- x: bfloat16 [4096, 4096], P(('dp', 'cp'))
- k_cache: bfloat16 [4096, 2, 128], P(('dp', 'cp'), 'tp')
- v_cache: bfloat16 [4096, 2, 128], P(('dp', 'cp'), 'tp')
- rope_table: float32 [4096, 64], P(('dp', 'cp'))
- norm_gain: bfloat16 [4096], replicated
- w_qkv: bfloat16 [4096, 4608], P(None, 'tp')
- b_qkv: bfloat16 [4608], P('tp')
- w_out: bfloat16 [4096, 4096], P('tp')
Outputs:
- output 1: bfloat16 [4096, 4096], P(('dp', 'cp'))
- output 2: bfloat16 [4096, 2, 128], P(('dp', 'cp'), 'tp')
- output 3: bfloat16 [4096, 2, 128], P(('dp', 'cp'), 'tp')
All inputs are finite; a program needn't handle non-finite values.
Results may differ from the reference program's by a relative error of at most 0.004026.
Values are sent between devices in bfloat16 or wider.
A program may use at most 1 GiB of HBM per device.

```python
import math
import jax
import jax.numpy as jnp
from jax import lax

D = 4096
HEADS = 32
KV_HEADS = 2
HEAD = 128
NEW_TOKENS = 4096
PREFIX = 4096
EPS = 1.5625e-07
MASK_VALUE = -1e30
GROUP = HEADS // KV_HEADS
QKV_WIDTH = (HEADS + 2 * KV_HEADS) * HEAD
PAIR_COUNT = HEAD // 4
QUERY_BLOCK = math.gcd(NEW_TOKENS, 128)
KEY_BLOCK = math.gcd(PREFIX + NEW_TOKENS, 512)


def setup_inputs(seed: int = 0, part: int = 0) -> dict:
    part_keys = jax.random.split(jax.random.fold_in(jax.random.key(seed), part), 4)
    shared_keys = jax.random.split(jax.random.key(seed + 1), 4)
    x = jax.random.normal(part_keys[0], (NEW_TOKENS, D), jnp.float32)
    k_cache = 1.6 * jax.random.normal(part_keys[1], (PREFIX, KV_HEADS, HEAD), jnp.float32)
    v_cache = 1.6 * jax.random.normal(part_keys[2], (PREFIX, KV_HEADS, HEAD), jnp.float32)
    log_ratio = jax.random.uniform(part_keys[3], (), jnp.float32, math.log(100.0), math.log(10000.0))
    rope_base = 10000.0 * jnp.exp(log_ratio)
    inv_freq = rope_base ** (-jnp.arange(PAIR_COUNT, dtype=jnp.float32) / PAIR_COUNT)
    positions = (PREFIX + jnp.arange(NEW_TOKENS)).astype(jnp.float32)
    angles = positions[:, None] * inv_freq[None, :]
    rope_table = jnp.concatenate([jnp.cos(angles), jnp.sin(angles)], axis=1)
    norm_gain = 1.0 + 0.3 * jax.random.normal(shared_keys[0], (D,), jnp.float32)
    w_qkv = jax.random.normal(shared_keys[1], (D, QKV_WIDTH), jnp.float32) * (1.5 / math.sqrt(D))
    b_qkv = 0.5 * jax.random.normal(shared_keys[2], (QKV_WIDTH,), jnp.float32)
    w_out = jax.random.normal(shared_keys[3], (HEADS * HEAD, D), jnp.float32) / math.sqrt(HEADS * HEAD)
    return dict(x=x.astype(jnp.bfloat16), k_cache=k_cache.astype(jnp.bfloat16), v_cache=v_cache.astype(jnp.bfloat16), rope_table=rope_table.astype(jnp.float32), norm_gain=norm_gain.astype(jnp.bfloat16), w_qkv=w_qkv.astype(jnp.bfloat16), b_qkv=b_qkv.astype(jnp.bfloat16), w_out=w_out.astype(jnp.bfloat16))


def apply_rotary(vals, cos_t, sin_t):
    pair_count = cos_t.shape[-1]
    lead_shape = vals.shape[:-1]
    paired = vals[..., :2 * pair_count].reshape(lead_shape + (pair_count, 2))
    even_part = paired[..., 0]
    odd_part = paired[..., 1]
    turned = jnp.stack([even_part * cos_t - odd_part * sin_t, odd_part * cos_t + even_part * sin_t], axis=-1)
    return jnp.concatenate([turned.reshape(lead_shape + (2 * pair_count,)), vals[..., 2 * pair_count:]], axis=-1)


def reference(x, k_cache, v_cache, rope_table, norm_gain, w_qkv, b_qkv, w_out):
    x_f32 = x.astype(jnp.float32)
    inv_rms = lax.rsqrt(jnp.mean(x_f32 * x_f32, axis=-1, keepdims=True) + EPS)
    hidden = (x_f32 * inv_rms * norm_gain.astype(jnp.float32)).astype(jnp.bfloat16)
    qkv_all = jnp.dot(hidden, w_qkv, preferred_element_type=jnp.float32) + b_qkv.astype(jnp.float32)
    qkv_all = qkv_all.reshape(NEW_TOKENS, KV_HEADS, GROUP + 2, HEAD)
    cos_t = rope_table[:, :PAIR_COUNT]
    sin_t = rope_table[:, PAIR_COUNT:]
    queries = apply_rotary(qkv_all[:, :, :GROUP], cos_t[:, None, None], sin_t[:, None, None]).astype(jnp.bfloat16)
    new_k = apply_rotary(qkv_all[:, :, GROUP], cos_t[:, None], sin_t[:, None]).astype(jnp.bfloat16)
    new_v = qkv_all[:, :, GROUP + 1].astype(jnp.bfloat16)
    key_count = PREFIX + NEW_TOKENS
    key_blocks = key_count // KEY_BLOCK
    keys_all = jnp.concatenate([k_cache, new_k], axis=0).reshape(key_blocks, KEY_BLOCK, KV_HEADS, HEAD)
    vals_all = jnp.concatenate([v_cache, new_v], axis=0).reshape(key_blocks, KEY_BLOCK, KV_HEADS, HEAD)
    key_pos = jnp.arange(key_count).reshape(key_blocks, KEY_BLOCK)
    q_blocks = queries.reshape(NEW_TOKENS // QUERY_BLOCK, QUERY_BLOCK, KV_HEADS, GROUP, HEAD)
    q_pos = (PREFIX + jnp.arange(NEW_TOKENS)).reshape(NEW_TOKENS // QUERY_BLOCK, QUERY_BLOCK)
    scale = HEAD ** -0.5

    def query_block(block):
        q_vals, q_at = block
        q_f32 = q_vals.astype(jnp.float32)

        def key_step(carry, kv_block):
            run_max, run_sum, weighted = carry
            k_vals, v_vals, k_at = kv_block
            scores = jnp.einsum('qngd,knd->qngk', q_f32, k_vals.astype(jnp.float32)) * scale
            visible = (k_at[None, :] <= q_at[:, None])[:, None, None, :]
            scores = jnp.where(visible, scores, MASK_VALUE)
            new_max = jnp.maximum(run_max, scores.max(axis=-1))
            rescale = jnp.exp(run_max - new_max)
            probs = jnp.exp(scores - new_max[..., None])
            run_sum = run_sum * rescale + probs.sum(axis=-1)
            weighted = weighted * rescale[..., None] + jnp.einsum('qngk,knd->qngd', probs.astype(jnp.bfloat16).astype(jnp.float32), v_vals.astype(jnp.float32))
            return (new_max, run_sum, weighted), None

        start_carry = (jnp.full((QUERY_BLOCK, KV_HEADS, GROUP), MASK_VALUE, jnp.float32), jnp.zeros((QUERY_BLOCK, KV_HEADS, GROUP), jnp.float32), jnp.zeros((QUERY_BLOCK, KV_HEADS, GROUP, HEAD), jnp.float32))
        (run_max, run_sum, weighted), _ = lax.scan(key_step, start_carry, (keys_all, vals_all, key_pos))
        return weighted / run_sum[..., None]

    attn = lax.map(query_block, (q_blocks, q_pos))
    attn = attn.reshape(NEW_TOKENS, HEADS * HEAD).astype(jnp.bfloat16)
    y = (x_f32 + jnp.dot(attn, w_out, preferred_element_type=jnp.float32)).astype(jnp.bfloat16)
    return y, new_k, new_v
```

```python
import functools
import math

import jax
import jax.numpy as jnp
from jax import lax
from jax.experimental import pallas as pl
from jax.experimental.pallas import tpu as pltpu
from jax.sharding import PartitionSpec as P

EPS = 1.5625e-07
NEG = -1e30
HEAD = 128
SCALE2 = HEAD ** -0.5 * math.log2(math.e)
F32 = jnp.float32
BF = jnp.bfloat16
VMEM_LIMIT = 60 * 2 ** 20


def rotate(a, cos, sin):
    lane = lax.broadcasted_iota(jnp.int32, a.shape, 1)
    other = jnp.where(lane % 2 == 0, pltpu.roll(a, HEAD - 1, 1), pltpu.roll(a, 1, 1))
    return a * cos + other * sin


def norm_kv_kernel(x_ref, g_ref, w_ref, b_ref, cos_ref, sin_ref, h_ref, k_ref, v_ref):
    x = x_ref[...].astype(F32)
    inv = lax.rsqrt(jnp.mean(x * x, axis=-1, keepdims=True) + EPS)
    h = (x * inv * g_ref[...].astype(F32)).astype(BF)
    h_ref[...] = h
    a = jnp.dot(h, w_ref[...], preferred_element_type=F32) + b_ref[...].astype(F32)
    k_ref[...] = rotate(a[:, :HEAD], cos_ref[...], sin_ref[...]).astype(BF)
    v_ref[...] = a[:, HEAD:].astype(BF)


def norm_kv(x, g, w_qkv, b, cos, sin, block=128):
    rows, d = x.shape
    last = w_qkv.shape[1] // (2 * HEAD) - 1
    row = lambda i: (i, 0)
    return pl.pallas_call(
        norm_kv_kernel,
        grid=(rows // block,),
        in_specs=[
            pl.BlockSpec((block, d), row),
            pl.BlockSpec((1, d), lambda i: (0, 0)),
            pl.BlockSpec((d, 2 * HEAD), lambda i: (0, last)),
            pl.BlockSpec((1, 2 * HEAD), lambda i: (0, last)),
            pl.BlockSpec((block, HEAD), row),
            pl.BlockSpec((block, HEAD), row),
        ],
        out_specs=[pl.BlockSpec((block, d), row), pl.BlockSpec((block, HEAD), row), pl.BlockSpec((block, HEAD), row)],
        out_shape=[jax.ShapeDtypeStruct((rows, d), BF), jax.ShapeDtypeStruct((rows, HEAD), BF), jax.ShapeDtypeStruct((rows, HEAD), BF)],
        compiler_params=pltpu.CompilerParams(dimension_semantics=("arbitrary",), vmem_limit_bytes=VMEM_LIMIT),
        cost_estimate=pl.CostEstimate(flops=2 * rows * d * 2 * HEAD, bytes_accessed=4 * rows * d, transcendentals=0),
        name="norm_kv",
    )(x, g, w_qkv, b, cos, sin)


def q_kernel(h_ref, w_ref, b_ref, cos_ref, sin_ref, q_ref):
    a = jnp.dot(h_ref[...], w_ref[...], preferred_element_type=F32) + b_ref[...].astype(F32)
    for i in range(a.shape[1] // HEAD):
        at = slice(i * HEAD, (i + 1) * HEAD)
        q_ref[:, at] = rotate(a[:, at], cos_ref[...], sin_ref[...]).astype(BF)


def q_proj(h, w_qkv, b, cos, sin, width, block=256):
    rows, d = h.shape
    return pl.pallas_call(
        q_kernel,
        grid=(width // block,),
        in_specs=[
            pl.BlockSpec((rows, d), lambda i: (0, 0)),
            pl.BlockSpec((d, block), lambda i: (0, i)),
            pl.BlockSpec((1, block), lambda i: (0, i)),
            pl.BlockSpec((rows, HEAD), lambda i: (0, 0)),
            pl.BlockSpec((rows, HEAD), lambda i: (0, 0)),
        ],
        out_specs=pl.BlockSpec((rows, block), lambda i: (0, i)),
        out_shape=jax.ShapeDtypeStruct((rows, width), BF),
        compiler_params=pltpu.CompilerParams(dimension_semantics=("arbitrary",), vmem_limit_bytes=VMEM_LIMIT),
        cost_estimate=pl.CostEstimate(flops=2 * rows * d * width, bytes_accessed=2 * d * width, transcendentals=0),
        name="q_proj",
    )(h, w_qkv, b, cos, sin)


def attn_kernel(c_ref, q_ref, qn_ref, k_ref, vt_ref, o_ref, s_ref, p_ref, acc_ref, mx_ref, *, bk, ch, rows):
    h = pl.program_id(0)
    half = rows // 2
    nfull = (4096 + rows * c_ref[0]) // bk
    own = 4096 + 3 * rows
    n = bk // ch

    def qk(qr, base, u, lo, width):
        k = k_ref[pl.ds(base + u * ch, ch), :]
        s = lax.dot_general(k, qr[pl.ds(lo, width), :], (((1,), (1,)), ((), ())), preferred_element_type=F32)
        s_ref[pl.ds(u * ch, ch), pl.ds(lo, width)] = s
        return s.reshape(ch // 8, 8, width).max(axis=0)

    def stage(ep, carry_m, carry_l, mx8, pv, nqk, masked=None):
        lo, width = ep
        m_new = jnp.maximum(carry_m, mx8.max(axis=0, keepdims=True))
        alpha = jnp.exp2((carry_m - m_new) * SCALE2)
        l8 = carry_l * alpha
        tot = None
        nmx = None
        for u in range(n):
            def do_pv(tot):
                if pv is None: return tot
                pb, plo, pw, _ = pv
                x = jnp.dot(vt_ref[:, pl.ds(pb + u * ch, ch)], p_ref[pl.ds(u * ch, ch), pl.ds(plo, pw)], preferred_element_type=F32)
                return x if tot is None else tot + x
            def do_exp(l8):
                s = s_ref[pl.ds(u * ch, ch), pl.ds(lo, width)]
                if masked is not None:
                    kk = lax.broadcasted_iota(jnp.int32, (ch, width), 0) + (u * ch)
                    qq = lax.broadcasted_iota(jnp.int32, (ch, width), 1)
                    s = jnp.where(kk <= qq, s, NEG)
                p = jnp.exp2((s - m_new) * SCALE2)
                l8 = l8 + p.reshape(ch // 8, 8, width).sum(axis=0)
                p_ref[pl.ds(u * ch, ch), pl.ds(lo, width)] = p.astype(BF)
                return l8
            def do_qk(nmx):
                if nqk is None: return nmx
                x = qk(nqk[0], nqk[1], u, nqk[2], nqk[3])
                return x if nmx is None else jnp.maximum(nmx, x)
            tot = do_pv(tot)
            l8 = do_exp(l8)
            nmx = do_qk(nmx)
        if pv is not None:
            _, plo, pw, pal = pv
            acc_ref[:, pl.ds(plo, pw)] = acc_ref[:, pl.ds(plo, pw)] * pal + tot
        return m_new, l8, nmx, alpha

    def first_mx():
        mx = None
        for u in range(n):
            x = qk(q_ref, 0, u, 0, rows)
            mx = x if mx is None else jnp.maximum(mx, x)
        mx_ref[...] = mx

    @pl.when(h == 0)
    def _():
        first_mx()
        p_ref[...] = jnp.zeros_like(p_ref)
        acc_ref[...] = jnp.zeros_like(acc_ref)

    m0 = jnp.full((1, rows), NEG, F32)
    z1 = jnp.zeros((1, rows), F32)
    z8 = jnp.zeros((8, rows), F32)

    def body(j, carry):
        m, l8, mx8, al = carry
        pb = pl.multiple_of(jnp.maximum(j - 1, 0) * bk, bk)
        nb = pl.multiple_of(jnp.where(j == nfull - 1, own, (j + 1) * bk), bk)
        return stage((0, rows), m, l8, mx8, (pb, 0, rows, al), (q_ref, nb, 0, rows))
    m, l8, mx8, al = lax.fori_loop(0, nfull, body, (m0, z8, mx_ref[...], z1))

    kk = lax.broadcasted_iota(jnp.int32, (half, half), 0)
    qq = lax.broadcasted_iota(jnp.int32, (half, half), 1)
    s_ref[:, pl.ds(0, half)] = jnp.where(kk <= qq, s_ref[:, pl.ds(0, half)], NEG)
    lastb = pl.multiple_of((nfull - 1) * bk, bk)
    m, l8, mx8b, al = stage((0, rows), m, l8, mx8, (lastb, 0, rows, al), (q_ref, own + half, half, half))
    mr, lr = m[:, half:], l8[:, half:]
    s_ref[:, pl.ds(half, half)] = jnp.where(kk <= qq, s_ref[:, pl.ds(half, half)], NEG)
    mr, lr, _, alr = stage((half, half), mr, lr, mx8b, (own, 0, rows, al), None)
    tot = None
    for u in range(n):
        x = jnp.dot(vt_ref[:, pl.ds(own + half + u * ch, ch)], p_ref[pl.ds(u * ch, ch), pl.ds(half, half)], preferred_element_type=F32)
        tot = x if tot is None else tot + x
    right = acc_ref[:, pl.ds(half, half)] * alr + tot
    mx = None
    for u in range(n):
        x = qk(qn_ref, 0, u, 0, rows)
        mx = x if mx is None else jnp.maximum(mx, x)
    mx_ref[...] = mx
    inv_l = l8[:, :half].sum(axis=0, keepdims=True)
    inv_r = lr.sum(axis=0, keepdims=True)
    o_ref[pl.ds(0, half), :] = (acc_ref[:, pl.ds(0, half)] / inv_l).astype(BF).T
    o_ref[pl.ds(half, half), :] = (right / inv_r).astype(BF).T

def attention(c, q, k_all, vt_all, *, heads, h0=0, bk=512, ch=256, rows=1024):
    kern = functools.partial(attn_kernel, bk=bk, ch=ch, rows=rows)
    nk = k_all.shape[0]
    return pl.pallas_call(
        kern,
        grid_spec=pltpu.PrefetchScalarGridSpec(
            num_scalar_prefetch=1, grid=(heads,),
            in_specs=[pl.BlockSpec((rows, 128), lambda h, c: (0, h + h0)),
                      pl.BlockSpec((rows, 128), lambda h, c: (0, jnp.minimum(h + 1, heads - 1) + h0)),
                      pl.BlockSpec((nk, 128), lambda h, c: (0, 0)),
                      pl.BlockSpec((128, nk), lambda h, c: (0, 0))],
            out_specs=pl.BlockSpec((rows, 128), lambda h, c: (0, h)),
            scratch_shapes=[pltpu.VMEM((bk, rows), F32), pltpu.VMEM((bk, rows), BF), pltpu.VMEM((128, rows), F32), pltpu.VMEM((8, rows), F32)]),
        out_shape=jax.ShapeDtypeStruct((rows, heads * 128), BF),
        compiler_params=pltpu.CompilerParams(dimension_semantics=("arbitrary",), vmem_limit_bytes=VMEM_LIMIT),
        cost_estimate=pl.CostEstimate(flops=4 * rows * heads * HEAD * nk, bytes_accessed=4 * rows * heads * HEAD, transcendentals=rows * heads * nk),
        name="attention",
    )(c, q, q, k_all, vt_all)


def own_kernel(x_ref, o_refs, w_ref, y_ref):
    total = x_ref[...].astype(F32)
    step = w_ref.shape[0] // len(o_refs)
    for i, o_ref in enumerate(o_refs):
        total += jnp.dot(o_ref[...], w_ref[pl.ds(i * step, step), :], preferred_element_type=F32)
    y_ref[...] = total


def own_part(x, o_parts, w, block=512):
    rows, d = x.shape
    depth = w.shape[0]
    col = lambda i: (0, i)
    return pl.pallas_call(
        lambda x_ref, *rest: own_kernel(x_ref, rest[:-2], rest[-2], rest[-1]),
        grid=(d // block,),
        in_specs=[pl.BlockSpec((rows, block), col)]
        + [pl.BlockSpec(o.shape, lambda i: (0, 0)) for o in o_parts]
        + [pl.BlockSpec((depth, block), col)],
        out_specs=pl.BlockSpec((rows, block), col),
        out_shape=jax.ShapeDtypeStruct((rows, d), F32),
        compiler_params=pltpu.CompilerParams(dimension_semantics=("arbitrary",), vmem_limit_bytes=VMEM_LIMIT),
        cost_estimate=pl.CostEstimate(flops=2 * rows * d * depth, bytes_accessed=6 * rows * d, transcendentals=0),
        name="own_part",
    )(x, *o_parts, w)


def other_kernel(idx_ref, y_ref, *rest, parts):
    o_refs, w_refs, out_ref, o_buf = rest[:parts], rest[parts:2 * parts], rest[2 * parts], rest[2 * parts + 1]
    width = o_refs[0].shape[1]

    @pl.when(pl.program_id(0) == 0)
    def _():
        for i, o_ref in enumerate(o_refs):
            o_buf[:, pl.ds(i * width, width)] = o_ref[...]

    total = y_ref[...]
    for i, w_ref in enumerate(w_refs):
        at = pl.multiple_of(idx_ref[i] * width, width)
        total += jnp.dot(o_buf[:, pl.ds(at, width)], w_ref[...], preferred_element_type=F32)
    out_ref[...] = total.astype(BF)


def other_part(idx, y, o_parts, w_parts, block=512):
    rows, d = y.shape
    parts = len(o_parts)
    col = lambda i, idx: (0, i)
    depth = w_parts[0].shape[0] * parts
    return pl.pallas_call(
        functools.partial(other_kernel, parts=parts),
        grid_spec=pltpu.PrefetchScalarGridSpec(
            num_scalar_prefetch=1,
            grid=(d // block,),
            in_specs=[pl.BlockSpec((rows, block), col)]
            + [pl.BlockSpec(o.shape, lambda i, idx: (0, 0)) for o in o_parts]
            + [pl.BlockSpec((w.shape[0], block), col) for w in w_parts],
            out_specs=pl.BlockSpec((rows, block), col),
            scratch_shapes=[pltpu.VMEM((rows, depth), BF)],
        ),
        out_shape=jax.ShapeDtypeStruct((rows, d), BF),
        compiler_params=pltpu.CompilerParams(dimension_semantics=("arbitrary",), vmem_limit_bytes=VMEM_LIMIT),
        cost_estimate=pl.CostEstimate(flops=2 * rows * d * depth, bytes_accessed=6 * rows * d, transcendentals=0),
        name="other_part",
    )(idx, y, *o_parts, *w_parts)


def rope_tables(table):
    pairs = table.shape[1] // 2
    pair = jnp.arange(HEAD) // 2
    hot = (jnp.arange(pairs)[:, None] == pair[None, :]).astype(F32)
    sign = jnp.where(jnp.arange(HEAD) % 2 == 0, -1.0, 1.0)
    spread = lambda a, b: jnp.dot(a, b, precision=lax.Precision.HIGHEST, preferred_element_type=F32)
    stay = (pair >= pairs).astype(F32)
    return spread(table[:, :pairs], hot) + stay, spread(table[:, pairs:], hot * sign)


def shift(a, by, n):
    return lax.ppermute(a, "cp", [(i, (i + by) % n) for i in range(n)])


def flip(a, bits, n):
    return lax.ppermute(a, "cp", [(i, i ^ bits) for i in range(n)])


CALLS = 4


def local_step(x, k_cache, v_cache, rope_table, norm_gain, w_qkv, b_qkv, w_out):
    rows = x.shape[0]
    n = lax.axis_size("cp")
    c = lax.axis_index("cp")
    swap = [(0, 1), (1, 0)]
    width = w_out.shape[0]
    heads = width // HEAD
    quarter = width // n

    kv_cache = jnp.concatenate([k_cache[:, 0], v_cache[:, 0]], axis=0)
    old = [kv_cache] + [shift(kv_cache, s, n) for s in range(1, n)]
    w_mine = lax.dynamic_slice_in_dim(w_out, c * quarter, quarter, 0)
    w_peer = lax.ppermute(w_mine, "tp", swap)

    cos, sin = rope_tables(rope_table)
    bias = b_qkv[None]
    h, new_k, new_v = norm_kv(x, norm_gain[None], w_qkv, bias, cos, sin)
    kv_new = jnp.concatenate([new_k, new_v], axis=0)
    new = [shift(kv_new, s, n) for s in range(1, n)] + [kv_new]
    queries = q_proj(h, w_qkv, bias, cos, sin, width)

    k_all = jnp.concatenate([a[:rows] for a in old + new], axis=0)
    vt_all = jnp.concatenate([a[rows:] for a in old + new], axis=0).T

    where = c.astype(jnp.int32)[None]
    per = heads // CALLS
    o_own, o_other = [], []
    for i in range(CALLS):
        part = attention(where, queries, k_all, vt_all, heads=per, h0=i * per)
        o_own.append(part)
        o_other.append(lax.ppermute(part, "tp", swap))
    w_x = flip(w_peer, 2, n)
    w_parts = [w_peer, flip(w_peer, 1, n), w_x, flip(w_x, 1, n)]
    idx = jnp.stack([c, c ^ 1, c ^ 2, c ^ 3]).astype(jnp.int32)

    y = own_part(x, o_own, w_out)
    y = other_part(idx, y, o_other, w_parts)
    return y, new_k[:, None], new_v[:, None]


def solution(mesh):
    row_spec = P(("dp", "cp"), None)
    cache_spec = P(("dp", "cp"), "tp", None)
    return jax.shard_map(
        local_step,
        mesh=mesh,
        in_specs=(row_spec, cache_spec, cache_spec, row_spec, P(None), P(None, "tp"), P("tp"), P("tp", None)),
        out_specs=(row_spec, cache_spec, cache_spec),
        check_vma=False,
    )
```

```python
import functools
import math

import jax
import jax.numpy as jnp
from jax import lax
from jax.experimental import pallas as pl
from jax.experimental.pallas import tpu as pltpu
from jax.sharding import PartitionSpec as P


EPS = 1.5625e-07
NEG = -1e30
HEAD = 128
SCALE2 = HEAD ** -0.5 * math.log2(math.e)
F32 = jnp.float32
BF = jnp.bfloat16
VMEM_LIMIT = 60 * 2 ** 20
ATTN_VMEM = 24 * 2 ** 20


def rotate(a, cos, sin):
    lane = lax.broadcasted_iota(jnp.int32, a.shape, 1)
    other = jnp.where(lane % 2 == 0, pltpu.roll(a, HEAD - 1, 1), pltpu.roll(a, 1, 1))
    return a * cos + other * sin


def norm_kv_kernel(x_ref, g_ref, w_ref, b_ref, cos_ref, sin_ref, h_ref, k_ref, v_ref):
    for r in range(x_ref.shape[0] // 128):
        rs = pl.ds(r * 128, 128)
        x = x_ref[rs, :].astype(F32)
        inv = lax.rsqrt(jnp.mean(x * x, axis=-1, keepdims=True) + EPS)
        h = (x * inv * g_ref[...].astype(F32)).astype(BF)
        h_ref[rs, :] = h
        a = jnp.dot(h, w_ref[...], preferred_element_type=F32) + b_ref[...].astype(F32)
        k_ref[rs, :] = rotate(a[:, :HEAD], cos_ref[rs, :], sin_ref[rs, :]).astype(BF)
        v_ref[rs, :] = a[:, HEAD:].astype(BF)


def norm_kv(x, g, w_qkv, b, cos, sin, block=256):
    rows, d = x.shape
    last = w_qkv.shape[1] // (2 * HEAD) - 1
    row = lambda i: (i, 0)
    return pl.pallas_call(
        norm_kv_kernel,
        grid=(rows // block,),
        in_specs=[
            pl.BlockSpec((block, d), row),
            pl.BlockSpec((1, d), lambda i: (0, 0)),
            pl.BlockSpec((d, 2 * HEAD), lambda i: (0, last)),
            pl.BlockSpec((1, 2 * HEAD), lambda i: (0, last)),
            pl.BlockSpec((block, HEAD), row),
            pl.BlockSpec((block, HEAD), row),
        ],
        out_specs=[pl.BlockSpec((block, d), row), pl.BlockSpec((block, HEAD), row), pl.BlockSpec((block, HEAD), row)],
        out_shape=[jax.ShapeDtypeStruct((rows, d), BF), jax.ShapeDtypeStruct((rows, HEAD), BF), jax.ShapeDtypeStruct((rows, HEAD), BF)],
        compiler_params=pltpu.CompilerParams(dimension_semantics=("arbitrary",), vmem_limit_bytes=VMEM_LIMIT),
        cost_estimate=pl.CostEstimate(flops=2 * rows * d * 2 * HEAD, bytes_accessed=4 * rows * d, transcendentals=0),
        name="norm_kv",
    )(x, g, w_qkv, b, cos, sin)


def q_kernel(h_ref, w_ref, b_ref, cos_ref, sin_ref, q_ref):
    for r in range(h_ref.shape[0] // 128):
        rs = pl.ds(r * 128, 128)
        a = jnp.dot(h_ref[rs, :], w_ref[...], preferred_element_type=F32) + b_ref[...].astype(F32)
        for i in range(a.shape[1] // HEAD):
            at = slice(i * HEAD, (i + 1) * HEAD)
            q_ref[rs, at] = rotate(a[:, at], cos_ref[rs, :], sin_ref[rs, :]).astype(BF)


def q_proj(h, w_qkv, b, cos, sin, width, block=512):
    rows, d = h.shape
    return pl.pallas_call(
        q_kernel,
        grid=(width // block,),
        in_specs=[
            pl.BlockSpec((rows, d), lambda i: (0, 0)),
            pl.BlockSpec((d, block), lambda i: (0, i)),
            pl.BlockSpec((1, block), lambda i: (0, i)),
            pl.BlockSpec((rows, HEAD), lambda i: (0, 0)),
            pl.BlockSpec((rows, HEAD), lambda i: (0, 0)),
        ],
        out_specs=pl.BlockSpec((rows, block), lambda i: (0, i)),
        out_shape=jax.ShapeDtypeStruct((rows, width), BF),
        compiler_params=pltpu.CompilerParams(dimension_semantics=("arbitrary",), vmem_limit_bytes=VMEM_LIMIT),
        cost_estimate=pl.CostEstimate(flops=2 * rows * d * width, bytes_accessed=2 * d * width, transcendentals=0),
        name="q_proj",
    )(h, w_qkv, b, cos, sin)


HEADS = 16
MOVED = 3


def given(cp):
    return jnp.where(cp == 3, MOVED, jnp.where(cp == 2, 1, 0))


def taken(cp):
    return given(3 - cp)


STRIP = 256
CHUNK = 256


def attn_kernel(cp_ref, q_ref, qn_ref, k_ref, vt_ref, *rest, old, first, foreign):
    back_ref = rest[0] if len(rest) == 9 else None
    o_ref, s_ref, p_ref, acc_ref, mx_ref, m_ref, l_ref, al_ref = rest[-8:]
    slot = pl.program_id(0)
    rows = q_ref.shape[0]
    strips = rows // STRIP
    chunks = rows // CHUNK
    cp = cp_ref[0]
    if foreign:
        owner = jnp.where(slot < taken(cp), 3 - cp, -1)
    else:
        owner = jnp.where(first + slot < HEADS - given(cp), cp, -1)

    def scores(qr, base, u, w):
        k = k_ref[pl.ds(base + u * CHUNK, CHUNK), :]
        return lax.dot_general(k, qr[pl.ds(w * STRIP, STRIP), :], (((1,), (1,)), ((), ())), preferred_element_type=F32)

    def col_max(s):
        return s.reshape(CHUNK // 8, 8, STRIP).max(axis=0)

    def triangle(s):
        key = lax.broadcasted_iota(jnp.int32, s.shape, 0)
        query = lax.broadcasted_iota(jnp.int32, s.shape, 1)
        return jnp.where(key <= query, s, NEG)

    def product(base, u, w):
        at = base // HEAD + u * (CHUNK // HEAD)
        vt = jnp.concatenate([vt_ref[at + i] for i in range(CHUNK // HEAD)], axis=1)
        p = jnp.concatenate([p_ref[w * (STRIP // HEAD) + i, pl.ds(u * CHUNK, CHUNK), :] for i in range(STRIP // HEAD)], axis=1)
        return jnp.dot(vt, p, preferred_element_type=F32)

    def stage(ex=None, pv=None, qk=None, diagonal=False):
        for w in range(strips):
            ne = ex[w] if ex else 0
            np_ = pv[1][w] if pv else 0
            nq = qk[2][w] if qk else 0
            cs = pl.ds(w * STRIP, STRIP)
            total = None
            top = None
            if ne:
                m_old = m_ref[0:1, cs]
                m_new = jnp.maximum(m_old, mx_ref[:, cs].max(axis=0, keepdims=True))
                alpha = jnp.exp2((m_old - m_new) * SCALE2)
                l8 = l_ref[:, cs] * alpha
            for u in range(chunks):
                ks = pl.ds(u * CHUNK, CHUNK)
                if u < np_:
                    x = product(pv[0], u, w)
                    total = x if total is None else total + x
                if u < ne:
                    e = jnp.exp2((s_ref[ks, cs] - m_new) * SCALE2)
                    l8 = l8 + e.reshape(CHUNK // 8, 8, STRIP).sum(axis=0)
                    e = e.astype(BF)
                    for i in range(STRIP // HEAD):
                        p_ref[w * (STRIP // HEAD) + i, ks, :] = e[:, i * HEAD:(i + 1) * HEAD]
                if u < nq:
                    s = scores(qk[0], qk[1], u, w)
                    if diagonal and u == nq - 1:
                        s = triangle(s)
                    s_ref[ks, cs] = s
                    x = col_max(s)
                    top = x if top is None else jnp.maximum(top, x)
            if np_:
                acc_ref[:, cs] = acc_ref[:, cs] * al_ref[0:1, cs] + total
            if ne:
                m_ref[:, cs] = jnp.broadcast_to(m_new, (8, STRIP))
                al_ref[:, cs] = jnp.broadcast_to(alpha, (8, STRIP))
                l_ref[:, cs] = l8
            if nq:
                mx_ref[:, cs] = top

    full = [chunks] * strips
    upper = [w + 1 for w in range(strips)]

    @pl.when((slot == 0) & (owner >= 0))
    def _():
        stage(qk=(q_ref, 0, full))
        p_ref[...] = jnp.zeros_like(p_ref)
        acc_ref[...] = jnp.zeros_like(acc_ref)

    @pl.when(owner >= 0)
    def _():
        own = pl.multiple_of(old + rows * owner, rows)
        m_ref[...] = jnp.full_like(m_ref, NEG)
        l_ref[...] = jnp.zeros_like(l_ref)
        al_ref[...] = jnp.zeros_like(al_ref)

        def body(j, carry):
            before = pl.multiple_of(jnp.maximum(j - 1, 0) * rows, rows)
            after = pl.multiple_of((j + 1) * rows, rows)
            stage(full, (before, full), (q_ref, after, full))
            return carry

        lax.fori_loop(0, own // rows - 1, body, 0)
        stage(full, (pl.multiple_of(own - 2 * rows, rows), full), (q_ref, own, upper), diagonal=True)
        stage(upper, (pl.multiple_of(own - rows, rows), full), (qn_ref, 0, full))
        stage(pv=(own, upper))
        for w in range(strips):
            cs = pl.ds(w * STRIP, STRIP)
            o_ref[cs, :] = (acc_ref[:, cs] / l_ref[:, cs].sum(axis=0, keepdims=True)).astype(BF).T

    if back_ref is not None:
        @pl.when(owner < 0)
        def _():
            o_ref[...] = back_ref[...]


def attention(cp, q, k_all, vt_all, *, slots, first=0, foreign=False, back=None):
    rows = q.shape[0]
    keys = k_all.shape[0]
    old = keys - 4 * rows
    if foreign:
        col = lambda s: slots - 1 - s
    else:
        col = lambda s: s + first
    row_block = lambda index: pl.BlockSpec((rows, HEAD), index)
    operands = [q, q, k_all, vt_all]
    in_specs = [
        row_block(lambda s, c: (0, col(s))),
        row_block(lambda s, c: (0, col(jnp.minimum(s + 1, slots - 1)))),
        pl.BlockSpec((keys, HEAD), lambda s, c: (0, 0)),
        pl.BlockSpec((keys // HEAD, HEAD, HEAD), lambda s, c: (0, 0, 0)),
    ]
    if back is not None:
        skip = slots - MOVED
        operands.append(back)
        in_specs.append(row_block(lambda s, c: (0, jnp.maximum(s - skip, 0))))
    return pl.pallas_call(
        functools.partial(attn_kernel, old=old, first=first, foreign=foreign),
        grid_spec=pltpu.PrefetchScalarGridSpec(
            num_scalar_prefetch=1,
            grid=(slots,),
            in_specs=in_specs,
            out_specs=row_block(lambda s, c: (0, col(s) if foreign else s)),
            scratch_shapes=[
                pltpu.VMEM((rows, rows), F32),
                pltpu.VMEM((rows // HEAD, rows, HEAD), BF),
                pltpu.VMEM((HEAD, rows), F32),
            ]
            + [pltpu.VMEM((8, rows), F32)] * 4,
        ),
        out_shape=jax.ShapeDtypeStruct((rows, slots * HEAD), BF),
        compiler_params=pltpu.CompilerParams(dimension_semantics=("arbitrary",), vmem_limit_bytes=ATTN_VMEM),
        cost_estimate=pl.CostEstimate(flops=4 * rows * slots * HEAD * keys, bytes_accessed=4 * rows * slots * HEAD, transcendentals=0),
        name="attention",
    )(cp, *operands)


def gather_kernel(cp_ref, *refs):
    parts, (k_ref, vt_ref) = refs[:-2], refs[-2:]
    rows = k_ref.shape[0]
    for i, part in enumerate(parts):
        @pl.when(pl.program_id(0) == i)
        def _(part=part):
            k_ref[...] = part[pl.ds(0, rows), :]
            for b in range(rows // HEAD):
                vt_ref[b] = part[pl.ds(rows + b * HEAD, HEAD), :].T


def gather(cp, old, new):
    n = len(old)
    rows = old[0].shape[0] // 2
    place = lambda i, c: (i // n) * n + lax.rem(c[0] + n - lax.rem(i, n), n)
    return pl.pallas_call(
        gather_kernel,
        grid_spec=pltpu.PrefetchScalarGridSpec(
            num_scalar_prefetch=1,
            grid=(2 * n,),
            in_specs=[pl.BlockSpec((2 * rows, HEAD), lambda i, c: (0, 0))] * (2 * n),
            out_specs=[
                pl.BlockSpec((rows, HEAD), lambda i, c: (place(i, c), 0)),
                pl.BlockSpec((rows // HEAD, HEAD, HEAD), lambda i, c: (place(i, c), 0, 0)),
            ],
        ),
        out_shape=[
            jax.ShapeDtypeStruct((2 * n * rows, HEAD), BF),
            jax.ShapeDtypeStruct((2 * n * rows // HEAD, HEAD, HEAD), BF),
        ],
        compiler_params=pltpu.CompilerParams(dimension_semantics=("arbitrary",), vmem_limit_bytes=ATTN_VMEM),
        cost_estimate=pl.CostEstimate(flops=2 ** 20, bytes_accessed=2 ** 23, transcendentals=0),
        name="gather",
    )(cp, *old, *new)


def own_kernel(x_ref, *rest):
    o_refs, w_ref, y_ref = rest[:-2], rest[-2], rest[-1]
    for r in range(x_ref.shape[0] // 256):
        rs = pl.ds(r * 256, 256)
        o = jnp.concatenate([o_ref[rs, :] for o_ref in o_refs], axis=1)
        y_ref[rs, :] = x_ref[rs, :].astype(F32) + jnp.dot(o, w_ref[...], preferred_element_type=F32)


def own_part(x, o_parts, w, block=512):
    rows, d = x.shape
    depth = w.shape[0]
    col = lambda i: (0, i)
    return pl.pallas_call(
        own_kernel,
        grid=(d // block,),
        in_specs=[pl.BlockSpec((rows, block), col)]
        + [pl.BlockSpec(o.shape, lambda i: (0, 0)) for o in o_parts]
        + [pl.BlockSpec((depth, block), col)],
        out_specs=pl.BlockSpec((rows, block), col),
        out_shape=jax.ShapeDtypeStruct((rows, d), F32),
        compiler_params=pltpu.CompilerParams(dimension_semantics=("arbitrary",), vmem_limit_bytes=VMEM_LIMIT),
        cost_estimate=pl.CostEstimate(flops=2 * rows * d * depth, bytes_accessed=6 * rows * d, transcendentals=0),
        name="own_part",
    )(x, *o_parts, w)


def other_kernel(cp_ref, y_ref, *rest, parts):
    o_refs, w_refs, out_ref, o_buf = rest[:parts], rest[parts:-2], rest[-2], rest[-1]

    @pl.when(pl.program_id(0) == 0)
    def _():
        at = 0
        for o_ref in o_refs:
            o_buf[:, pl.ds(at, o_ref.shape[1])] = o_ref[...]
            at += o_ref.shape[1]

    depth = w_refs[0].shape[0]
    halves = len(w_refs) // 4
    for r in range(y_ref.shape[0] // 256):
        rs = pl.ds(r * 256, 256)
        total = None
        for i, w_ref in enumerate(w_refs):
            at = pl.multiple_of(((cp_ref[0] ^ (i // halves)) * halves + i % halves) * depth, depth)
            x = jnp.dot(o_buf[rs, pl.ds(at, depth)], w_ref[...], preferred_element_type=F32)
            total = x if total is None else total + x
        out_ref[rs, :] = (y_ref[rs, :] + total).astype(BF)


def other_part(cp, y, o_parts, w_parts, block=512):
    rows, d = y.shape
    col = lambda i, c: (0, i)
    depth = sum(w.shape[0] for w in w_parts)
    return pl.pallas_call(
        functools.partial(other_kernel, parts=len(o_parts)),
        grid_spec=pltpu.PrefetchScalarGridSpec(
            num_scalar_prefetch=1,
            grid=(d // block,),
            in_specs=[pl.BlockSpec((rows, block), col)]
            + [pl.BlockSpec(o.shape, lambda i, c: (0, 0)) for o in o_parts]
            + [pl.BlockSpec((w.shape[0], block), col) for w in w_parts],
            out_specs=pl.BlockSpec((rows, block), col),
            scratch_shapes=[pltpu.VMEM((rows, depth), BF)],
        ),
        out_shape=jax.ShapeDtypeStruct((rows, d), BF),
        compiler_params=pltpu.CompilerParams(dimension_semantics=("arbitrary",), vmem_limit_bytes=VMEM_LIMIT),
        cost_estimate=pl.CostEstimate(flops=2 * rows * d * depth, bytes_accessed=6 * rows * d, transcendentals=0),
        name="other_part",
    )(cp, y, *o_parts, *w_parts)


def rope_tables(table):
    pairs = table.shape[1] // 2
    pair = jnp.arange(HEAD) // 2
    hot = (jnp.arange(pairs)[:, None] == pair[None, :]).astype(F32)
    sign = jnp.where(jnp.arange(HEAD) % 2 == 0, -1.0, 1.0)
    spread = lambda a, b: jnp.dot(a, b, precision=lax.Precision.HIGHEST, preferred_element_type=F32)
    stay = (pair >= pairs).astype(F32)
    return spread(table[:, :pairs], hot) + stay, spread(table[:, pairs:], hot * sign)


SIZES = (4, 5, 3, 4)
PIECES = 2


def after(a, *others):
    return lax.optimization_barrier((a, *others))[0]


def local_step(x, k_cache, v_cache, rope_table, norm_gain, w_qkv, b_qkv, w_out):
    n = lax.axis_size("cp")
    cp = lax.axis_index("cp")
    swap = [(0, 1), (1, 0)]
    width = w_out.shape[0]
    piece = width // (n * PIECES)
    where = cp.astype(jnp.int32)[None]
    around = lambda s: [(i, (i + s) % n) for i in range(n)]
    flip = lambda bits: [(i, i ^ bits) for i in range(n)]

    kv_cache = jnp.concatenate([k_cache[:, 0], v_cache[:, 0]], axis=0)
    old = [kv_cache] + [lax.ppermute(kv_cache, "cp", around(s)) for s in range(1, n)]
    w_peer = []
    for i in range(PIECES):
        mine = lax.dynamic_slice_in_dim(w_out, (cp * PIECES + i) * piece, piece, 0)
        w_peer.append(lax.ppermute(mine, "tp", swap))

    cos, sin = rope_tables(rope_table)
    bias = b_qkv[None]
    h, new_k, new_v = norm_kv(x, norm_gain[None], w_qkv, bias, cos, sin)
    kv_new = jnp.concatenate([new_k, new_v], axis=0)
    new = [kv_new] + [lax.ppermute(kv_new, "cp", around(s)) for s in range(1, n)]
    queries = q_proj(h, w_qkv, bias, cos, sin, width)
    q_far = lax.ppermute(queries[:, width - MOVED * HEAD:], "cp", [(3, 0), (2, 1)])

    k_all, vt_all = gather(where, old, new)
    attend = functools.partial(attention, where, k_all=k_all, vt_all=vt_all)

    o_own, o_other = [], []

    def heads(i, *previous, back=None):
        q = after(queries, *previous) if previous else queries
        part = attend(q=q, slots=SIZES[i], first=sum(SIZES[:i]), back=back)
        o_own.append(part)
        o_other.append(lax.ppermute(part, "tp", swap))
        return part

    part = heads(0)
    w_peer = [after(w, part) for w in w_peer]
    w_x = [lax.ppermute(w, "cp", flip(2)) for w in w_peer]
    w_core = [lax.ppermute(w, "cp", flip(1)) for w in w_peer]
    far = attend(q=after(q_far, part), slots=MOVED, foreign=True)
    part = heads(1, far)
    back = lax.ppermute(far, "cp", [(0, 3), (1, 2)])
    part = heads(2, part)
    part = heads(3, part, back=back)
    w_x = [after(w, part) for w in w_x]
    w_far = [lax.ppermute(w, "cp", flip(1)) for w in w_x]

    y = own_part(x, o_own, w_out)
    y = other_part(where, y, o_other, [*w_peer, *w_core, *w_x, *w_far])
    return y, new_k[:, None], new_v[:, None]


def solution(mesh):
    row_spec = P(("dp", "cp"), None)
    cache_spec = P(("dp", "cp"), "tp", None)
    return jax.shard_map(
        local_step,
        mesh=mesh,
        in_specs=(row_spec, cache_spec, cache_spec, row_spec, P(None), P(None, "tp"), P("tp"), P("tp", None)),
        out_specs=(row_spec, cache_spec, cache_spec),
        check_vma=False,
    )
```

```python
import functools
import math

import jax
import jax.numpy as jnp
from jax import lax
from jax.experimental import pallas as pl
from jax.experimental.pallas import tpu as pltpu
from jax.sharding import PartitionSpec as P


EPS = 1.5625e-07
NEG = -1e30
HEAD = 128
SCALE2 = HEAD ** -0.5 * math.log2(math.e)
F32 = jnp.float32
BF = jnp.bfloat16
VMEM_LIMIT = 60 * 2 ** 20
ATTN_VMEM = 24 * 2 ** 20
NORM_VMEM = 28 * 2 ** 20
Q_VMEM = 36 * 2 ** 20


def rotate(a, cos, sin):
    lane = lax.broadcasted_iota(jnp.int32, a.shape, 1)
    other = jnp.where(lane % 2 == 0, pltpu.roll(a, HEAD - 1, 1), pltpu.roll(a, 1, 1))
    return a * cos + other * sin


def norm_kv_kernel(cp_ref, x_ref, g_ref, w_ref, b_ref, table_ref, piece_ref, h_ref, kv_ref, k_ref, v_ref, cos_ref, sin_ref, copy_ref):
    copy_ref[...] = piece_ref[...]
    pairs = table_ref.shape[1] // 2
    lane = lax.broadcasted_iota(jnp.int32, (pairs, HEAD), 1)
    hit = lax.broadcasted_iota(jnp.int32, (pairs, HEAD), 0) == lane // 2
    spread = functools.partial(jnp.dot, precision=lax.Precision.HIGHEST, preferred_element_type=F32)
    stay = lax.broadcasted_iota(jnp.int32, (128, HEAD), 1) >= 2 * pairs
    for r in range(x_ref.shape[0] // 128):
        rs = pl.ds(r * 128, 128)
        table = table_ref[rs, :]
        cos = jnp.where(stay, 1.0, spread(table[:, :pairs], hit.astype(F32)))
        sin = spread(table[:, pairs:], jnp.where(hit, jnp.where(lane % 2 == 0, -1.0, 1.0), 0.0))
        cos_ref[rs, :] = cos
        sin_ref[rs, :] = sin
        x = x_ref[rs, :].astype(F32)
        inv = lax.rsqrt(jnp.mean(x * x, axis=-1, keepdims=True) + EPS)
        h = (x * inv * g_ref[...].astype(F32)).astype(BF)
        h_ref[rs, :] = h
        a = jnp.dot(h, w_ref[...], preferred_element_type=F32) + b_ref[...].astype(F32)
        k = rotate(a[:, :HEAD], cos, sin).astype(BF)
        v = a[:, HEAD:].astype(BF)
        k_ref[rs, :] = k
        v_ref[rs, :] = v
        kv_ref[0, rs, :] = k
        kv_ref[1, rs, :] = v


def norm_kv(cp, x, g, w_qkv, b, table, w_out, piece, block=256):
    rows, d = x.shape
    steps = rows // block
    last = w_qkv.shape[1] // (2 * HEAD) - 1
    row = lambda i, c: (i, 0)
    part = piece // steps
    head_rows = pl.BlockSpec((block, HEAD), row)
    return pl.pallas_call(
        norm_kv_kernel,
        grid_spec=pltpu.PrefetchScalarGridSpec(
            num_scalar_prefetch=1,
            grid=(steps,),
            in_specs=[
                pl.BlockSpec((block, d), row),
                pl.BlockSpec((1, d), lambda i, c: (0, 0)),
                pl.BlockSpec((d, 2 * HEAD), lambda i, c: (0, last)),
                pl.BlockSpec((1, 2 * HEAD), lambda i, c: (0, last)),
                pl.BlockSpec((block, table.shape[1]), row),
                pl.BlockSpec((part, w_out.shape[1]), lambda i, c: ((c[0] * PIECES + 1) * steps + i, 0)),
            ],
            out_specs=[
                pl.BlockSpec((block, d), row),
                pl.BlockSpec((2, block, HEAD), lambda i, c: (0, i, 0)),
                head_rows,
                head_rows,
                head_rows,
                head_rows,
                pl.BlockSpec((part, w_out.shape[1]), row),
            ],
        ),
        out_shape=[
            jax.ShapeDtypeStruct((rows, d), BF),
            jax.ShapeDtypeStruct((2, rows, HEAD), BF),
            jax.ShapeDtypeStruct((rows, HEAD), BF),
            jax.ShapeDtypeStruct((rows, HEAD), BF),
            jax.ShapeDtypeStruct((rows, HEAD), F32),
            jax.ShapeDtypeStruct((rows, HEAD), F32),
            jax.ShapeDtypeStruct((piece, w_out.shape[1]), BF),
        ],
        compiler_params=pltpu.CompilerParams(dimension_semantics=("arbitrary",), vmem_limit_bytes=NORM_VMEM),
        cost_estimate=pl.CostEstimate(flops=2 * rows * d * 2 * HEAD, bytes_accessed=4 * rows * d, transcendentals=0),
        name="norm_kv",
    )(cp, x, g, w_qkv, b, table, w_out)


def q_kernel(h_ref, w_ref, b_ref, cos_ref, sin_ref, q_ref, far_ref):
    lead = far_ref.shape[1] - w_ref.shape[1]
    for r in range(h_ref.shape[0] // 128):
        rs = pl.ds(r * 128, 128)
        a = jnp.dot(h_ref[rs, :], w_ref[...], preferred_element_type=F32) + b_ref[...].astype(F32)
        for i in range(a.shape[1] // HEAD):
            at = slice(i * HEAD, (i + 1) * HEAD)
            q = rotate(a[:, at], cos_ref[rs, :], sin_ref[rs, :]).astype(BF)
            q_ref[rs, at] = q
            if i * HEAD + lead >= 0:
                far_ref[rs, pl.ds(i * HEAD + lead, HEAD)] = q


def q_proj(h, w_qkv, b, cos, sin, width, block=512):
    rows, d = h.shape
    far = MOVED * HEAD
    return pl.pallas_call(
        q_kernel,
        grid=(width // block,),
        in_specs=[
            pl.BlockSpec((rows, d), lambda i: (0, 0)),
            pl.BlockSpec((d, block), lambda i: (0, i)),
            pl.BlockSpec((1, block), lambda i: (0, i)),
            pl.BlockSpec((rows, HEAD), lambda i: (0, 0)),
            pl.BlockSpec((rows, HEAD), lambda i: (0, 0)),
        ],
        out_specs=[pl.BlockSpec((rows, block), lambda i: (0, i)), pl.BlockSpec((rows, far), lambda i: (0, 0))],
        out_shape=[jax.ShapeDtypeStruct((rows, width), BF), jax.ShapeDtypeStruct((rows, far), BF)],
        compiler_params=pltpu.CompilerParams(dimension_semantics=("arbitrary",), vmem_limit_bytes=Q_VMEM),
        cost_estimate=pl.CostEstimate(flops=2 * rows * d * width, bytes_accessed=2 * d * width, transcendentals=0),
        name="q_proj",
    )(h, w_qkv, b, cos, sin)


HEADS = 16
MOVED = 3


def given(cp):
    return jnp.where(cp == 3, MOVED, jnp.where(cp == 2, 1, 0))


def taken(cp):
    return given(3 - cp)


STRIP = 256
CHUNK = 256


def attn_kernel(cp_ref, q_ref, qn_ref, k_ref, vt_ref, *rest, old, first, foreign):
    back_ref = rest[0] if len(rest) == 9 else None
    o_ref, s_ref, p_ref, acc_ref, mx_ref, m_ref, l_ref, al_ref = rest[-8:]
    slot = pl.program_id(0)
    rows = q_ref.shape[0]
    strips = rows // STRIP
    chunks = rows // CHUNK
    cp = cp_ref[0]
    if foreign:
        owner = jnp.where(slot < taken(cp), 3 - cp, -1)
    else:
        owner = jnp.where(first + slot < HEADS - given(cp), cp, -1)

    def scores(qr, base, u, w):
        k = k_ref[pl.ds(base + u * CHUNK, CHUNK), :]
        return lax.dot_general(k, qr[pl.ds(w * STRIP, STRIP), :], (((1,), (1,)), ((), ())), preferred_element_type=F32)

    def col_max(s):
        return s.reshape(CHUNK // 8, 8, STRIP).max(axis=0)

    def triangle(s):
        key = lax.broadcasted_iota(jnp.int32, s.shape, 0)
        query = lax.broadcasted_iota(jnp.int32, s.shape, 1)
        return jnp.where(key <= query, s, NEG)

    def product(base, u, w):
        at = base // HEAD + u * (CHUNK // HEAD)
        vt = jnp.concatenate([vt_ref[at + i] for i in range(CHUNK // HEAD)], axis=1)
        p = jnp.concatenate([p_ref[w * (STRIP // HEAD) + i, pl.ds(u * CHUNK, CHUNK), :] for i in range(STRIP // HEAD)], axis=1)
        return jnp.dot(vt, p, preferred_element_type=F32)

    def stage(ex=None, pv=None, qk=None, diagonal=False):
        for w in range(strips):
            ne = ex[w] if ex else 0
            np_ = pv[1][w] if pv else 0
            nq = qk[2][w] if qk else 0
            cs = pl.ds(w * STRIP, STRIP)
            total = None
            top = None
            if ne:
                m_old = m_ref[0:1, cs]
                m_new = jnp.maximum(m_old, mx_ref[:, cs].max(axis=0, keepdims=True))
                alpha = jnp.exp2((m_old - m_new) * SCALE2)
                l8 = l_ref[:, cs] * alpha
            for u in range(chunks):
                ks = pl.ds(u * CHUNK, CHUNK)
                if u < np_:
                    x = product(pv[0], u, w)
                    total = x if total is None else total + x
                if u < ne:
                    e = jnp.exp2((s_ref[ks, cs] - m_new) * SCALE2)
                    l8 = l8 + e.reshape(CHUNK // 8, 8, STRIP).sum(axis=0)
                    e = e.astype(BF)
                    for i in range(STRIP // HEAD):
                        p_ref[w * (STRIP // HEAD) + i, ks, :] = e[:, i * HEAD:(i + 1) * HEAD]
                if u < nq:
                    s = scores(qk[0], qk[1], u, w)
                    if diagonal and u == nq - 1:
                        s = triangle(s)
                    s_ref[ks, cs] = s
                    x = col_max(s)
                    top = x if top is None else jnp.maximum(top, x)
            if np_:
                acc_ref[:, cs] = acc_ref[:, cs] * al_ref[0:1, cs] + total
            if ne:
                m_ref[:, cs] = jnp.broadcast_to(m_new, (8, STRIP))
                al_ref[:, cs] = jnp.broadcast_to(alpha, (8, STRIP))
                l_ref[:, cs] = l8
            if nq:
                mx_ref[:, cs] = top

    full = [chunks] * strips
    upper = [w + 1 for w in range(strips)]

    @pl.when((slot == 0) & (owner >= 0))
    def _():
        stage(qk=(q_ref, 0, full))
        p_ref[...] = jnp.zeros_like(p_ref)
        acc_ref[...] = jnp.zeros_like(acc_ref)

    @pl.when(owner >= 0)
    def _():
        own = pl.multiple_of(old + rows * owner, rows)
        m_ref[...] = jnp.full_like(m_ref, NEG)
        l_ref[...] = jnp.zeros_like(l_ref)
        al_ref[...] = jnp.zeros_like(al_ref)

        def body(j, carry):
            before = pl.multiple_of(jnp.maximum(j - 1, 0) * rows, rows)
            after = pl.multiple_of((j + 1) * rows, rows)
            stage(full, (before, full), (q_ref, after, full))
            return carry

        lax.fori_loop(0, own // rows - 1, body, 0)
        stage(full, (pl.multiple_of(own - 2 * rows, rows), full), (q_ref, own, upper), diagonal=True)
        stage(upper, (pl.multiple_of(own - rows, rows), full), (qn_ref, 0, full))
        stage(pv=(own, upper))
        for w in range(strips):
            cs = pl.ds(w * STRIP, STRIP)
            o_ref[cs, :] = (acc_ref[:, cs] / l_ref[:, cs].sum(axis=0, keepdims=True)).astype(BF).T

    if back_ref is not None:
        @pl.when(owner < 0)
        def _():
            o_ref[...] = back_ref[...]


def attention(cp, q, k_all, vt_all, *, slots, first=0, foreign=False, back=None):
    rows = q.shape[0]
    keys = k_all.shape[0]
    old = keys - 4 * rows
    if foreign:
        col = lambda s: slots - 1 - s
    else:
        col = lambda s: s + first
    row_block = lambda index: pl.BlockSpec((rows, HEAD), index)
    operands = [q, q, k_all, vt_all]
    in_specs = [
        row_block(lambda s, c: (0, col(s))),
        row_block(lambda s, c: (0, col(jnp.minimum(s + 1, slots - 1)))),
        pl.BlockSpec((keys, HEAD), lambda s, c: (0, 0)),
        pl.BlockSpec((keys // HEAD, HEAD, HEAD), lambda s, c: (0, 0, 0)),
    ]
    if back is not None:
        skip = slots - MOVED
        operands.append(back)
        in_specs.append(row_block(lambda s, c: (0, jnp.maximum(s - skip, 0))))
    return pl.pallas_call(
        functools.partial(attn_kernel, old=old, first=first, foreign=foreign),
        grid_spec=pltpu.PrefetchScalarGridSpec(
            num_scalar_prefetch=1,
            grid=(slots,),
            in_specs=in_specs,
            out_specs=row_block(lambda s, c: (0, col(s) if foreign else s)),
            scratch_shapes=[
                pltpu.VMEM((rows, rows), F32),
                pltpu.VMEM((rows // HEAD, rows, HEAD), BF),
                pltpu.VMEM((HEAD, rows), F32),
            ]
            + [pltpu.VMEM((8, rows), F32)] * 4,
        ),
        out_shape=jax.ShapeDtypeStruct((rows, slots * HEAD), BF),
        compiler_params=pltpu.CompilerParams(dimension_semantics=("arbitrary",), vmem_limit_bytes=ATTN_VMEM),
        cost_estimate=pl.CostEstimate(flops=4 * rows * slots * HEAD * keys, bytes_accessed=4 * rows * slots * HEAD, transcendentals=0),
        name="attention",
    )(cp, *operands)


def gather_kernel(cp_ref, *refs):
    parts, (k_ref, vt_ref) = refs[:-2], refs[-2:]
    rows = k_ref.shape[0]
    for i, part in enumerate(parts):
        @pl.when(pl.program_id(0) == i)
        def _(part=part):
            k_ref[...] = part[pl.ds(0, rows), :]
            for b in range(rows // HEAD):
                vt_ref[b] = part[pl.ds(rows + b * HEAD, HEAD), :].T


def gather(cp, old, new):
    n = len(old)
    rows = old[0].shape[0] // 2
    place = lambda i, c: (i // n) * n + lax.rem(c[0] + n - lax.rem(i, n), n)
    return pl.pallas_call(
        gather_kernel,
        grid_spec=pltpu.PrefetchScalarGridSpec(
            num_scalar_prefetch=1,
            grid=(2 * n,),
            in_specs=[pl.BlockSpec((2 * rows, HEAD), lambda i, c: (0, 0))] * (2 * n),
            out_specs=[
                pl.BlockSpec((rows, HEAD), lambda i, c: (place(i, c), 0)),
                pl.BlockSpec((rows // HEAD, HEAD, HEAD), lambda i, c: (place(i, c), 0, 0)),
            ],
        ),
        out_shape=[
            jax.ShapeDtypeStruct((2 * n * rows, HEAD), BF),
            jax.ShapeDtypeStruct((2 * n * rows // HEAD, HEAD, HEAD), BF),
        ],
        compiler_params=pltpu.CompilerParams(dimension_semantics=("arbitrary",), vmem_limit_bytes=ATTN_VMEM),
        cost_estimate=pl.CostEstimate(flops=2 ** 20, bytes_accessed=2 ** 23, transcendentals=0),
        name="gather",
    )(cp, *old, *new)


def own_kernel(x_ref, *rest):
    o_refs, w_ref, y_ref = rest[:-2], rest[-2], rest[-1]
    for r in range(x_ref.shape[0] // 256):
        rs = pl.ds(r * 256, 256)
        o = jnp.concatenate([o_ref[rs, :] for o_ref in o_refs], axis=1)
        y_ref[rs, :] = x_ref[rs, :].astype(F32) + jnp.dot(o, w_ref[...], preferred_element_type=F32)


def own_part(x, o_parts, w, block=512):
    rows, d = x.shape
    depth = w.shape[0]
    col = lambda i: (0, i)
    return pl.pallas_call(
        own_kernel,
        grid=(d // block,),
        in_specs=[pl.BlockSpec((rows, block), col)]
        + [pl.BlockSpec(o.shape, lambda i: (0, 0)) for o in o_parts]
        + [pl.BlockSpec((depth, block), col)],
        out_specs=pl.BlockSpec((rows, block), col),
        out_shape=jax.ShapeDtypeStruct((rows, d), F32),
        compiler_params=pltpu.CompilerParams(dimension_semantics=("arbitrary",), vmem_limit_bytes=VMEM_LIMIT),
        cost_estimate=pl.CostEstimate(flops=2 * rows * d * depth, bytes_accessed=6 * rows * d, transcendentals=0),
        name="own_part",
    )(x, *o_parts, w)


def other_kernel(cp_ref, y_ref, *rest, parts):
    o_refs, w_refs, out_ref, o_buf = rest[:parts], rest[parts:-2], rest[-2], rest[-1]

    @pl.when(pl.program_id(0) == 0)
    def _():
        at = 0
        for o_ref in o_refs:
            o_buf[:, pl.ds(at, o_ref.shape[1])] = o_ref[...]
            at += o_ref.shape[1]

    depth = w_refs[0].shape[0]
    halves = len(w_refs) // 4
    for r in range(y_ref.shape[0] // 256):
        rs = pl.ds(r * 256, 256)
        total = None
        for i, w_ref in enumerate(w_refs):
            at = pl.multiple_of(((cp_ref[0] ^ (i // halves)) * halves + i % halves) * depth, depth)
            x = jnp.dot(o_buf[rs, pl.ds(at, depth)], w_ref[...], preferred_element_type=F32)
            total = x if total is None else total + x
        out_ref[rs, :] = (y_ref[rs, :] + total).astype(BF)


def other_part(cp, y, o_parts, w_parts, block=512):
    rows, d = y.shape
    col = lambda i, c: (0, i)
    depth = sum(w.shape[0] for w in w_parts)
    return pl.pallas_call(
        functools.partial(other_kernel, parts=len(o_parts)),
        grid_spec=pltpu.PrefetchScalarGridSpec(
            num_scalar_prefetch=1,
            grid=(d // block,),
            in_specs=[pl.BlockSpec((rows, block), col)]
            + [pl.BlockSpec(o.shape, lambda i, c: (0, 0)) for o in o_parts]
            + [pl.BlockSpec((w.shape[0], block), col) for w in w_parts],
            out_specs=pl.BlockSpec((rows, block), col),
            scratch_shapes=[pltpu.VMEM((rows, depth), BF)],
        ),
        out_shape=jax.ShapeDtypeStruct((rows, d), BF),
        compiler_params=pltpu.CompilerParams(dimension_semantics=("arbitrary",), vmem_limit_bytes=VMEM_LIMIT),
        cost_estimate=pl.CostEstimate(flops=2 * rows * d * depth, bytes_accessed=6 * rows * d, transcendentals=0),
        name="other_part",
    )(cp, y, *o_parts, *w_parts)


SIZES = (4, 5, 3, 4)
PIECES = 2


def after(a, *others):
    return lax.optimization_barrier((a, *others))[0]


def local_step(x, k_cache, v_cache, rope_table, norm_gain, w_qkv, b_qkv, w_out):
    rows = x.shape[0]
    n = lax.axis_size("cp")
    cp = lax.axis_index("cp")
    swap = [(0, 1), (1, 0)]
    width = w_out.shape[0]
    piece = width // (n * PIECES)
    where = cp.astype(jnp.int32)[None]
    around = lambda s: [(i, (i + s) % n) for i in range(n)]
    flip = lambda bits: [(i, i ^ bits) for i in range(n)]

    kv_cache = jnp.concatenate([k_cache[:, 0], v_cache[:, 0]], axis=0)
    old = [kv_cache] + [lax.ppermute(kv_cache, "cp", around(s)) for s in range(1, n)]
    mine = lax.dynamic_slice_in_dim(w_out, cp * PIECES * piece, piece, 0)
    w_peer = [lax.ppermute(mine, "tp", swap)]

    bias = b_qkv[None]
    h, kv_new, new_k, new_v, cos, sin, mine = norm_kv(where, x, norm_gain[None], w_qkv, bias, rope_table, w_out, piece)
    w_peer.append(lax.ppermute(mine, "tp", swap))
    kv_new = kv_new.reshape(2 * rows, HEAD)
    new = [kv_new] + [lax.ppermute(kv_new, "cp", around(s)) for s in range(1, n)]
    queries, q_far = q_proj(h, w_qkv, bias, cos, sin, width)
    q_far = lax.ppermute(q_far, "cp", [(3, 0), (2, 1)])
    w_peer[0] = after(w_peer[0], queries)

    k_all, vt_all = gather(where, old, new)
    attend = functools.partial(attention, where, k_all=k_all, vt_all=vt_all)

    o_own, o_other = [], []

    def heads(i, *previous, back=None):
        q = after(queries, *previous) if previous else queries
        part = attend(q=q, slots=SIZES[i], first=sum(SIZES[:i]), back=back)
        o_own.append(part)
        o_other.append(lax.ppermute(part, "tp", swap))
        return part

    w_x, w_core, w_far = [None] * PIECES, [None] * PIECES, [None] * PIECES

    def spread(i):
        w_x[i] = lax.ppermute(w_peer[i], "cp", flip(2))
        w_core[i] = lax.ppermute(w_peer[i], "cp", flip(1))

    def spread_on(i):
        w_far[i] = lax.ppermute(w_x[i], "cp", flip(1))

    spread(0)
    part = heads(0)
    far = attend(q=after(q_far, part), slots=MOVED, foreign=True)
    back = lax.ppermute(far, "cp", [(0, 3), (1, 2)])
    part = heads(1, far)
    w_peer[1] = after(w_peer[1], part)
    w_x[0] = after(w_x[0], part)
    spread(1)
    spread_on(0)
    part = heads(2, part)
    part = heads(3, part, back=back)
    w_x[1] = after(w_x[1], part)
    spread_on(1)

    y = own_part(x, o_own, w_out)
    y = other_part(where, y, o_other, [*w_peer, *w_core, *w_x, *w_far])
    return y, new_k[:, None], new_v[:, None]


def solution(mesh):
    row_spec = P(("dp", "cp"), None)
    cache_spec = P(("dp", "cp"), "tp", None)
    return jax.shard_map(
        local_step,
        mesh=mesh,
        in_specs=(row_spec, cache_spec, cache_spec, row_spec, P(None), P(None, "tp"), P("tp"), P("tp", None)),
        out_specs=(row_spec, cache_spec, cache_spec),
        check_vma=False,
    )
```

```python
import functools
import math

import jax
import jax.numpy as jnp
from jax import lax
from jax.experimental import pallas as pl
from jax.experimental.pallas import tpu as pltpu
from jax.sharding import PartitionSpec as P


EPS = 1.5625e-07
NEG = -1e30
HEAD = 128
SCALE2 = HEAD ** -0.5 * math.log2(math.e)
F32 = jnp.float32
BF = jnp.bfloat16
ATTN_VMEM = 24 * 2 ** 20
NORM_VMEM = 48 * 2 ** 20
Q_VMEM = 36 * 2 ** 20
OUT_VMEM = 28 * 2 ** 20


def rotate(a, cos, sin):
    lane = lax.broadcasted_iota(jnp.int32, a.shape, 1)
    other = jnp.where(lane % 2 == 0, pltpu.roll(a, HEAD - 1, 1), pltpu.roll(a, 1, 1))
    return a * cos + other * sin


def norm_kv_kernel(cp_ref, x_ref, g_ref, w_ref, b_ref, table_ref, piece_ref, h_ref, kv_ref, k_ref, v_ref, cos_ref, sin_ref, copy_ref):
    copy_ref[...] = piece_ref[...]
    pairs = table_ref.shape[1] // 2
    lane = lax.broadcasted_iota(jnp.int32, (pairs, HEAD), 1)
    hit = lax.broadcasted_iota(jnp.int32, (pairs, HEAD), 0) == lane // 2
    spread = functools.partial(jnp.dot, precision=lax.Precision.HIGHEST, preferred_element_type=F32)
    stay = lax.broadcasted_iota(jnp.int32, (128, HEAD), 1) >= 2 * pairs
    for r in range(x_ref.shape[0] // 128):
        rs = pl.ds(r * 128, 128)
        table = table_ref[rs, :]
        cos = jnp.where(stay, 1.0, spread(table[:, :pairs], hit.astype(F32)))
        sin = spread(table[:, pairs:], jnp.where(hit, jnp.where(lane % 2 == 0, -1.0, 1.0), 0.0))
        cos_ref[rs, :] = cos
        sin_ref[rs, :] = sin
        x = x_ref[rs, :].astype(F32)
        inv = lax.rsqrt(jnp.mean(x * x, axis=-1, keepdims=True) + EPS)
        h = (x * inv * g_ref[...].astype(F32)).astype(BF)
        h_ref[rs, :] = h
        a = jnp.dot(h, w_ref[...], preferred_element_type=F32) + b_ref[...].astype(F32)
        k = rotate(a[:, :HEAD], cos, sin).astype(BF)
        v = a[:, HEAD:].astype(BF)
        k_ref[rs, :] = k
        v_ref[rs, :] = v
        kv_ref[0, rs, :] = k
        kv_ref[1, rs, :] = v


def norm_kv(cp, x, g, w_qkv, b, table, w_out, piece, block=256):
    rows, d = x.shape
    steps = rows // block
    last = w_qkv.shape[1] // (2 * HEAD) - 1
    row = lambda i, c: (i, 0)
    part = piece // steps
    head_rows = pl.BlockSpec((block, HEAD), row)
    return pl.pallas_call(
        norm_kv_kernel,
        grid_spec=pltpu.PrefetchScalarGridSpec(
            num_scalar_prefetch=1,
            grid=(steps,),
            in_specs=[
                pl.BlockSpec((block, d), row),
                pl.BlockSpec((1, d), lambda i, c: (0, 0)),
                pl.BlockSpec((d, 2 * HEAD), lambda i, c: (0, last)),
                pl.BlockSpec((1, 2 * HEAD), lambda i, c: (0, last)),
                pl.BlockSpec((block, table.shape[1]), row),
                pl.BlockSpec((part, w_out.shape[1]), lambda i, c: ((c[0] * PIECES + 1) * steps + i, 0)),
            ],
            out_specs=[
                pl.BlockSpec((block, d), row),
                pl.BlockSpec((2, block, HEAD), lambda i, c: (0, i, 0)),
                head_rows,
                head_rows,
                head_rows,
                head_rows,
                pl.BlockSpec((part, w_out.shape[1]), row),
            ],
        ),
        out_shape=[
            jax.ShapeDtypeStruct((rows, d), BF),
            jax.ShapeDtypeStruct((2, rows, HEAD), BF),
            jax.ShapeDtypeStruct((rows, HEAD), BF),
            jax.ShapeDtypeStruct((rows, HEAD), BF),
            jax.ShapeDtypeStruct((rows, HEAD), F32),
            jax.ShapeDtypeStruct((rows, HEAD), F32),
            jax.ShapeDtypeStruct((piece, w_out.shape[1]), BF),
        ],
        compiler_params=pltpu.CompilerParams(dimension_semantics=("arbitrary",), vmem_limit_bytes=NORM_VMEM),
        cost_estimate=pl.CostEstimate(flops=2 * rows * d * 2 * HEAD, bytes_accessed=4 * rows * d, transcendentals=0),
        name="norm_kv",
    )(cp, x, g, w_qkv, b, table, w_out)


def q_kernel(h_ref, w_ref, b_ref, cos_ref, sin_ref, q_ref, far_ref):
    lead = far_ref.shape[1] - w_ref.shape[1]
    for r in range(h_ref.shape[0] // 128):
        rs = pl.ds(r * 128, 128)
        a = jnp.dot(h_ref[rs, :], w_ref[...], preferred_element_type=F32) + b_ref[...].astype(F32)
        for i in range(a.shape[1] // HEAD):
            at = slice(i * HEAD, (i + 1) * HEAD)
            q = rotate(a[:, at], cos_ref[rs, :], sin_ref[rs, :]).astype(BF)
            q_ref[rs, at] = q
            if i * HEAD + lead >= 0:
                far_ref[rs, pl.ds(i * HEAD + lead, HEAD)] = q


def q_proj(h, w_qkv, b, cos, sin, width, block=512):
    rows, d = h.shape
    far = MOVED * HEAD
    return pl.pallas_call(
        q_kernel,
        grid=(width // block,),
        in_specs=[
            pl.BlockSpec((rows, d), lambda i: (0, 0)),
            pl.BlockSpec((d, block), lambda i: (0, i)),
            pl.BlockSpec((1, block), lambda i: (0, i)),
            pl.BlockSpec((rows, HEAD), lambda i: (0, 0)),
            pl.BlockSpec((rows, HEAD), lambda i: (0, 0)),
        ],
        out_specs=[pl.BlockSpec((rows, block), lambda i: (0, i)), pl.BlockSpec((rows, far), lambda i: (0, 0))],
        out_shape=[jax.ShapeDtypeStruct((rows, width), BF), jax.ShapeDtypeStruct((rows, far), BF)],
        compiler_params=pltpu.CompilerParams(dimension_semantics=("arbitrary",), vmem_limit_bytes=Q_VMEM),
        cost_estimate=pl.CostEstimate(flops=2 * rows * d * width, bytes_accessed=2 * d * width, transcendentals=0),
        name="q_proj",
    )(h, w_qkv, b, cos, sin)


HEADS = 16
MOVED = 3


def given(cp):
    return jnp.where(cp == 3, MOVED, jnp.where(cp == 2, 1, 0))


def taken(cp):
    return given(3 - cp)


STRIP = 256
CHUNK = 256


def attn_kernel(cp_ref, q_ref, qn_ref, k_ref, vt_ref, *rest, old, first, foreign):
    back_refs = rest[:-8]
    o_ref, s_ref, p_ref, acc_ref, mx_ref, m_ref, l_ref, al_ref = rest[-8:]
    slot = pl.program_id(0)
    rows = q_ref.shape[0]
    strips = rows // STRIP
    chunks = rows // CHUNK
    cp = cp_ref[0]
    if foreign:
        owner = jnp.where(first + slot < taken(cp), 3 - cp, -1)
    else:
        owner = jnp.where(first + slot < HEADS - given(cp), cp, -1)

    def scores(qr, base, u, w):
        k = k_ref[pl.ds(base + u * CHUNK, CHUNK), :]
        return lax.dot_general(k, qr[pl.ds(w * STRIP, STRIP), :], (((1,), (1,)), ((), ())), preferred_element_type=F32)

    def col_max(s):
        return s.reshape(CHUNK // 8, 8, STRIP).max(axis=0)

    def triangle(s):
        key = lax.broadcasted_iota(jnp.int32, s.shape, 0)
        query = lax.broadcasted_iota(jnp.int32, s.shape, 1)
        return jnp.where(key <= query, s, NEG)

    def product(base, u, w):
        at = base // HEAD + u * (CHUNK // HEAD)
        vt = jnp.concatenate([vt_ref[at + i] for i in range(CHUNK // HEAD)], axis=1)
        p = jnp.concatenate([p_ref[w * (STRIP // HEAD) + i, pl.ds(u * CHUNK, CHUNK), :] for i in range(STRIP // HEAD)], axis=1)
        return jnp.dot(vt, p, preferred_element_type=F32)

    def stage(ex=None, pv=None, qk=None, diagonal=False):
        for w in range(strips):
            ne = ex[w] if ex else 0
            np_ = pv[1][w] if pv else 0
            nq = qk[2][w] if qk else 0
            cs = pl.ds(w * STRIP, STRIP)
            total = None
            top = None
            if ne:
                m_old = m_ref[0:1, cs]
                m_new = jnp.maximum(m_old, mx_ref[:, cs].max(axis=0, keepdims=True))
                alpha = jnp.exp2((m_old - m_new) * SCALE2)
                l8 = l_ref[:, cs] * alpha
            for u in range(chunks):
                ks = pl.ds(u * CHUNK, CHUNK)
                if u < np_:
                    x = product(pv[0], u, w)
                    total = x if total is None else total + x
                if u < ne:
                    e = jnp.exp2((s_ref[ks, cs] - m_new) * SCALE2)
                    l8 = l8 + e.reshape(CHUNK // 8, 8, STRIP).sum(axis=0)
                    e = e.astype(BF)
                    for i in range(STRIP // HEAD):
                        p_ref[w * (STRIP // HEAD) + i, ks, :] = e[:, i * HEAD:(i + 1) * HEAD]
                if u < nq:
                    s = scores(qk[0], qk[1], u, w)
                    if diagonal and u == nq - 1:
                        s = triangle(s)
                    s_ref[ks, cs] = s
                    x = col_max(s)
                    top = x if top is None else jnp.maximum(top, x)
            if np_:
                acc_ref[:, cs] = acc_ref[:, cs] * al_ref[0:1, cs] + total
            if ne:
                m_ref[:, cs] = jnp.broadcast_to(m_new, (8, STRIP))
                al_ref[:, cs] = jnp.broadcast_to(alpha, (8, STRIP))
                l_ref[:, cs] = l8
            if nq:
                mx_ref[:, cs] = top

    full = [chunks] * strips
    upper = [w + 1 for w in range(strips)]

    @pl.when((slot == 0) & (owner >= 0))
    def _():
        def strip(w, carry):
            cs = pl.ds(pl.multiple_of(w * STRIP, STRIP), STRIP)
            top = None
            for u in range(chunks):
                ks = pl.ds(u * CHUNK, CHUNK)
                s = lax.dot_general(k_ref[ks, :], q_ref[cs, :], (((1,), (1,)), ((), ())), preferred_element_type=F32)
                s_ref[ks, cs] = s
                top = col_max(s) if top is None else jnp.maximum(top, col_max(s))
            mx_ref[:, cs] = top
            return carry

        lax.fori_loop(0, strips, strip, 0)

        def clear(i, carry):
            p_ref[i] = jnp.zeros_like(p_ref[0])
            return carry

        lax.fori_loop(0, rows // HEAD, clear, 0)
        acc_ref[...] = jnp.zeros_like(acc_ref)

    @pl.when(owner >= 0)
    def _():
        own = pl.multiple_of(old + rows * owner, rows)
        m_ref[...] = jnp.full_like(m_ref, NEG)
        l_ref[...] = jnp.zeros_like(l_ref)
        al_ref[...] = jnp.zeros_like(al_ref)

        def body(j, carry):
            before = pl.multiple_of(jnp.maximum(j - 1, 0) * rows, rows)
            after = pl.multiple_of((j + 1) * rows, rows)
            stage(full, (before, full), (q_ref, after, full))
            return carry

        lax.fori_loop(0, own // rows - 1, body, 0)
        stage(full, (pl.multiple_of(own - 2 * rows, rows), full), (q_ref, own, upper), diagonal=True)
        stage(upper, (pl.multiple_of(own - rows, rows), full), (qn_ref, 0, full))
        stage(pv=(own, upper))
        for w in range(strips):
            cs = pl.ds(w * STRIP, STRIP)
            o_ref[cs, :] = (acc_ref[:, cs] / l_ref[:, cs].sum(axis=0, keepdims=True)).astype(BF).T

    for i, back_ref in enumerate(back_refs):
        @pl.when((owner < 0) & ((slot == pl.num_programs(0) - 1) == (i == 0)))
        def _(back_ref=back_ref):
            o_ref[...] = back_ref[...]


def attention(cp, q, k_all, vt_all, *, slots, first=0, foreign=False, back=()):
    rows = q.shape[0]
    keys = k_all.shape[0]
    old = keys - 4 * rows
    if foreign:
        col = lambda s: MOVED - 1 - first - s
    else:
        col = lambda s: s + first
    row_block = lambda index: pl.BlockSpec((rows, HEAD), index)
    operands = [q, q, k_all, vt_all]
    in_specs = [
        row_block(lambda s, c: (0, col(s))),
        row_block(lambda s, c: (0, col(jnp.minimum(s + 1, slots - 1)))),
        pl.BlockSpec((keys, HEAD), lambda s, c: (0, 0)),
        pl.BlockSpec((keys // HEAD, HEAD, HEAD), lambda s, c: (0, 0, 0)),
    ]
    for i, part in enumerate(back):
        operands.append(part)
        in_specs.append(row_block((lambda s, c: (0, 0)) if i == 0 else (lambda s, c: (0, jnp.clip(s - (slots - MOVED), 0, MOVED - 2)))))
    return pl.pallas_call(
        functools.partial(attn_kernel, old=old, first=first, foreign=foreign),
        grid_spec=pltpu.PrefetchScalarGridSpec(
            num_scalar_prefetch=1,
            grid=(slots,),
            in_specs=in_specs,
            out_specs=row_block(lambda s, c: (0, slots - 1 - s if foreign else s)),
            scratch_shapes=[
                pltpu.VMEM((rows, rows), F32),
                pltpu.VMEM((rows // HEAD, rows, HEAD), BF),
                pltpu.VMEM((HEAD, rows), F32),
            ]
            + [pltpu.VMEM((8, rows), F32)] * 4,
        ),
        out_shape=jax.ShapeDtypeStruct((rows, slots * HEAD), BF),
        compiler_params=pltpu.CompilerParams(dimension_semantics=("arbitrary",), vmem_limit_bytes=ATTN_VMEM),
        cost_estimate=pl.CostEstimate(flops=4 * rows * slots * HEAD * keys, bytes_accessed=4 * rows * slots * HEAD, transcendentals=0),
        name="attention",
    )(cp, *operands)


def gather_kernel(cp_ref, *refs):
    parts, (k_ref, vt_ref) = refs[:-2], refs[-2:]
    rows = k_ref.shape[0]
    for i, part in enumerate(parts):
        @pl.when(pl.program_id(0) == i)
        def _(part=part):
            k_ref[...] = part[pl.ds(0, rows), :]
            for b in range(rows // HEAD):
                vt_ref[b] = part[pl.ds(rows + b * HEAD, HEAD), :].T


def gather(cp, old, new):
    n = len(old)
    rows = old[0].shape[0] // 2
    place = lambda i, c: jnp.where(i < n, c[0] ^ i, n + lax.rem(c[0] + 2 * n - i, n))
    return pl.pallas_call(
        gather_kernel,
        grid_spec=pltpu.PrefetchScalarGridSpec(
            num_scalar_prefetch=1,
            grid=(2 * n,),
            in_specs=[pl.BlockSpec((2 * rows, HEAD), lambda i, c: (0, 0))] * (2 * n),
            out_specs=[
                pl.BlockSpec((rows, HEAD), lambda i, c: (place(i, c), 0)),
                pl.BlockSpec((rows // HEAD, HEAD, HEAD), lambda i, c: (place(i, c), 0, 0)),
            ],
        ),
        out_shape=[
            jax.ShapeDtypeStruct((2 * n * rows, HEAD), BF),
            jax.ShapeDtypeStruct((2 * n * rows // HEAD, HEAD, HEAD), BF),
        ],
        compiler_params=pltpu.CompilerParams(dimension_semantics=("arbitrary",), vmem_limit_bytes=ATTN_VMEM),
        cost_estimate=pl.CostEstimate(flops=2 ** 20, bytes_accessed=2 ** 23, transcendentals=0),
        name="gather",
    )(cp, *old, *new)


def own_kernel(x_ref, *rest):
    o_refs, w_ref, y_ref = rest[:-2], rest[-2], rest[-1]
    for r in range(x_ref.shape[0] // 256):
        rs = pl.ds(r * 256, 256)
        o = jnp.concatenate([o_ref[rs, :] for o_ref in o_refs], axis=1)
        y_ref[rs, :] = x_ref[rs, :].astype(F32) + jnp.dot(o, w_ref[...], preferred_element_type=F32)


def own_part(x, o_parts, w, block=512):
    rows, d = x.shape
    depth = w.shape[0]
    col = lambda i: (0, i)
    return pl.pallas_call(
        own_kernel,
        grid=(d // block,),
        in_specs=[pl.BlockSpec((rows, block), col)]
        + [pl.BlockSpec(o.shape, lambda i: (0, 0)) for o in o_parts]
        + [pl.BlockSpec((depth, block), col)],
        out_specs=pl.BlockSpec((rows, block), col),
        out_shape=jax.ShapeDtypeStruct((rows, d), F32),
        compiler_params=pltpu.CompilerParams(dimension_semantics=("arbitrary",), vmem_limit_bytes=OUT_VMEM),
        cost_estimate=pl.CostEstimate(flops=2 * rows * d * depth, bytes_accessed=6 * rows * d, transcendentals=0),
        name="own_part",
    )(x, *o_parts, w)


def other_kernel(cp_ref, y_ref, *rest, parts):
    o_refs, w_refs, out_ref, o_buf = rest[:parts], rest[parts:-2], rest[-2], rest[-1]

    @pl.when(pl.program_id(0) == 0)
    def _():
        at = 0
        for o_ref in o_refs:
            o_buf[:, pl.ds(at, o_ref.shape[1])] = o_ref[...]
            at += o_ref.shape[1]

    depth = w_refs[0].shape[0]
    halves = len(w_refs) // 4
    for r in range(y_ref.shape[0] // 256):
        rs = pl.ds(r * 256, 256)
        total = None
        for i, w_ref in enumerate(w_refs):
            at = pl.multiple_of(((cp_ref[0] ^ (i // halves)) * halves + i % halves) * depth, depth)
            x = jnp.dot(o_buf[rs, pl.ds(at, depth)], w_ref[...], preferred_element_type=F32)
            total = x if total is None else total + x
        out_ref[rs, :] = (y_ref[rs, :] + total).astype(BF)


def other_part(cp, y, o_parts, w_parts, block=512):
    rows, d = y.shape
    col = lambda i, c: (0, i)
    depth = sum(w.shape[0] for w in w_parts)
    return pl.pallas_call(
        functools.partial(other_kernel, parts=len(o_parts)),
        grid_spec=pltpu.PrefetchScalarGridSpec(
            num_scalar_prefetch=1,
            grid=(d // block,),
            in_specs=[pl.BlockSpec((rows, block), col)]
            + [pl.BlockSpec(o.shape, lambda i, c: (0, 0)) for o in o_parts]
            + [pl.BlockSpec((w.shape[0], block), col) for w in w_parts],
            out_specs=pl.BlockSpec((rows, block), col),
            scratch_shapes=[pltpu.VMEM((rows, depth), BF)],
        ),
        out_shape=jax.ShapeDtypeStruct((rows, d), BF),
        compiler_params=pltpu.CompilerParams(dimension_semantics=("arbitrary",), vmem_limit_bytes=OUT_VMEM),
        cost_estimate=pl.CostEstimate(flops=2 * rows * d * depth, bytes_accessed=6 * rows * d, transcendentals=0),
        name="other_part",
    )(cp, y, *o_parts, *w_parts)


SIZES = (4, 5, 3, 4)
PIECES = 2


def after(a, *others):
    return lax.optimization_barrier((a, *others))[0]


def local_step(x, k_cache, v_cache, rope_table, norm_gain, w_qkv, b_qkv, w_out):
    rows = x.shape[0]
    n = lax.axis_size("cp")
    cp = lax.axis_index("cp")
    swap = [(0, 1), (1, 0)]
    width = w_out.shape[0]
    piece = width // (n * PIECES)
    where = cp.astype(jnp.int32)[None]
    around = lambda s: [(i, (i + s) % n) for i in range(n)]
    flip = lambda bits: [(i, i ^ bits) for i in range(n)]

    kv_cache = jnp.concatenate([k_cache[:, 0], v_cache[:, 0]], axis=0)
    old = [kv_cache, lax.ppermute(kv_cache, "cp", flip(1)), lax.ppermute(kv_cache, "cp", flip(2))]
    mine = lax.dynamic_slice_in_dim(w_out, cp * PIECES * piece, piece, 0)
    w_peer = [lax.ppermute(mine, "tp", swap)]

    bias = b_qkv[None]
    h, kv_new, new_k, new_v, cos, sin, mine = norm_kv(where, x, norm_gain[None], w_qkv, bias, rope_table, w_out, piece)
    w_peer.append(lax.ppermute(mine, "tp", swap))
    old.append(lax.ppermute(after(old[2], kv_new), "cp", flip(1)))
    kv_new = kv_new.reshape(2 * rows, HEAD)
    new = [kv_new] + [lax.ppermute(kv_new, "cp", around(s)) for s in range(1, n)]
    queries, q_far = q_proj(h, w_qkv, bias, cos, sin, width)
    q_far = lax.ppermute(q_far, "cp", [(3, 0), (2, 1)])
    w_peer[0] = after(w_peer[0], queries)

    k_all, vt_all = gather(where, old, new)
    attend = functools.partial(attention, where, k_all=k_all, vt_all=vt_all)

    o_own, o_other = [], []

    def heads(i, *previous, back=()):
        q = after(queries, *previous) if previous else queries
        part = attend(q=q, slots=SIZES[i], first=sum(SIZES[:i]), back=back)
        o_own.append(part)
        o_other.append(lax.ppermute(part, "tp", swap))
        return part

    w_x, w_core, w_far = [None] * PIECES, [None] * PIECES, [None] * PIECES

    def spread(i):
        w_x[i] = lax.ppermute(w_peer[i], "cp", flip(2))
        w_core[i] = lax.ppermute(w_peer[i], "cp", flip(1))

    def spread_on(i):
        w_far[i] = lax.ppermute(w_x[i], "cp", flip(1))

    def moved(first, slots, *previous):
        far = attend(q=after(q_far, *previous), slots=slots, first=first, foreign=True)
        return far, lax.ppermute(far, "cp", [(0, 3), (1, 2)])

    spread(0)
    part = heads(0)
    far, back0 = moved(0, 1, part)
    w_peer[1] = after(w_peer[1], far)
    spread(1)
    part = heads(1, far)
    far, back1 = moved(1, MOVED - 1, part)
    part = heads(2, far)
    part = heads(3, part, back=(back0, back1))
    w_x = [after(w, part) for w in w_x]
    spread_on(0)
    spread_on(1)

    y = own_part(x, o_own, w_out)
    y = other_part(where, y, o_other, [*w_peer, *w_core, *w_x, *w_far])
    return y, new_k[:, None], new_v[:, None]


def solution(mesh):
    row_spec = P(("dp", "cp"), None)
    cache_spec = P(("dp", "cp"), "tp", None)
    return jax.shard_map(
        local_step,
        mesh=mesh,
        in_specs=(row_spec, cache_spec, cache_spec, row_spec, P(None), P(None, "tp"), P("tp"), P("tp", None)),
        out_specs=(row_spec, cache_spec, cache_spec),
        check_vma=False,
    )
```

```python
import functools
import math

import jax
import jax.numpy as jnp
from jax import lax
from jax.experimental import pallas as pl
from jax.experimental.pallas import tpu as pltpu
from jax.sharding import PartitionSpec as P


EPS = 1.5625e-07
NEG = -1e30
HEAD = 128
SCALE2 = HEAD ** -0.5 * math.log2(math.e)
F32 = jnp.float32
BF = jnp.bfloat16
ATTN_VMEM = 24 * 2 ** 20
NORM_VMEM = 36 * 2 ** 20
Q_VMEM = 36 * 2 ** 20
OUT_VMEM = 28 * 2 ** 20


def rotate(a, cos, sin):
    lane = lax.broadcasted_iota(jnp.int32, a.shape, 1)
    other = jnp.where(lane % 2 == 0, pltpu.roll(a, HEAD - 1, 1), pltpu.roll(a, 1, 1))
    return a * cos + other * sin


def norm_kv_kernel(cp_ref, x_ref, g_ref, w_ref, b_ref, table_ref, piece_ref, h_ref, kv_ref, k_ref, v_ref, cos_ref, sin_ref, copy_ref):
    copy_ref[...] = piece_ref[...]
    pairs = table_ref.shape[1] // 2
    lane = lax.broadcasted_iota(jnp.int32, (pairs, HEAD), 1)
    hit = lax.broadcasted_iota(jnp.int32, (pairs, HEAD), 0) == lane // 2
    spread = functools.partial(jnp.dot, precision=lax.Precision.HIGHEST, preferred_element_type=F32)
    stay = lax.broadcasted_iota(jnp.int32, (128, HEAD), 1) >= 2 * pairs
    for r in range(x_ref.shape[0] // 128):
        rs = pl.ds(r * 128, 128)
        table = table_ref[rs, :]
        cos = jnp.where(stay, 1.0, spread(table[:, :pairs], hit.astype(F32)))
        sin = spread(table[:, pairs:], jnp.where(hit, jnp.where(lane % 2 == 0, -1.0, 1.0), 0.0))
        cos_ref[rs, :] = cos
        sin_ref[rs, :] = sin
        x = x_ref[rs, :].astype(F32)
        inv = lax.rsqrt(jnp.mean(x * x, axis=-1, keepdims=True) + EPS)
        h = (x * inv * g_ref[...].astype(F32)).astype(BF)
        h_ref[rs, :] = h
        a = jnp.dot(h, w_ref[...], preferred_element_type=F32) + b_ref[...].astype(F32)
        k = rotate(a[:, :HEAD], cos, sin).astype(BF)
        v = a[:, HEAD:].astype(BF)
        k_ref[rs, :] = k
        v_ref[rs, :] = v
        kv_ref[0, rs, :] = k
        kv_ref[1, rs, :] = v


def norm_kv(cp, x, g, w_qkv, b, table, w_out, block=256):
    rows, d = x.shape
    steps = rows // block
    last = w_qkv.shape[1] // (2 * HEAD) - 1
    row = lambda i, c: (i, 0)
    skip, piece = PIECE_ROWS
    pieces = piece // skip
    copied = lambda i: jnp.minimum(i, pieces - 1)
    head_rows = pl.BlockSpec((block, HEAD), row)
    return pl.pallas_call(
        norm_kv_kernel,
        grid_spec=pltpu.PrefetchScalarGridSpec(
            num_scalar_prefetch=1,
            grid=(steps,),
            in_specs=[
                pl.BlockSpec((block, d), row),
                pl.BlockSpec((1, d), lambda i, c: (0, 0)),
                pl.BlockSpec((d, 2 * HEAD), lambda i, c: (0, last)),
                pl.BlockSpec((1, 2 * HEAD), lambda i, c: (0, last)),
                pl.BlockSpec((block, table.shape[1]), row),
                pl.BlockSpec((skip, w_out.shape[1]), lambda i, c: (c[0] * (pieces + 1) + 1 + copied(i), 0)),
            ],
            out_specs=[
                pl.BlockSpec((block, d), row),
                pl.BlockSpec((2, block, HEAD), lambda i, c: (0, i, 0)),
                head_rows,
                head_rows,
                head_rows,
                head_rows,
                pl.BlockSpec((skip, w_out.shape[1]), lambda i, c: (copied(i), 0)),
            ],
        ),
        out_shape=[
            jax.ShapeDtypeStruct((rows, d), BF),
            jax.ShapeDtypeStruct((2, rows, HEAD), BF),
            jax.ShapeDtypeStruct((rows, HEAD), BF),
            jax.ShapeDtypeStruct((rows, HEAD), BF),
            jax.ShapeDtypeStruct((rows, HEAD), F32),
            jax.ShapeDtypeStruct((rows, HEAD), F32),
            jax.ShapeDtypeStruct((piece, w_out.shape[1]), BF),
        ],
        compiler_params=pltpu.CompilerParams(dimension_semantics=("arbitrary",), vmem_limit_bytes=NORM_VMEM),
        cost_estimate=pl.CostEstimate(flops=2 * rows * d * 2 * HEAD, bytes_accessed=4 * rows * d, transcendentals=0),
        name="norm_kv",
    )(cp, x, g, w_qkv, b, table, w_out)


def q_kernel(h_ref, w_ref, b_ref, cos_ref, sin_ref, q_ref, far_ref):
    lead = far_ref.shape[1] - w_ref.shape[1]
    for r in range(h_ref.shape[0] // 128):
        rs = pl.ds(r * 128, 128)
        a = jnp.dot(h_ref[rs, :], w_ref[...], preferred_element_type=F32) + b_ref[...].astype(F32)
        for i in range(a.shape[1] // HEAD):
            at = slice(i * HEAD, (i + 1) * HEAD)
            q = rotate(a[:, at], cos_ref[rs, :], sin_ref[rs, :]).astype(BF)
            q_ref[rs, at] = q
            if i * HEAD + lead >= 0:
                far_ref[rs, pl.ds(i * HEAD + lead, HEAD)] = q


def q_proj(h, w_qkv, b, cos, sin, width, block=512):
    rows, d = h.shape
    far = MOVED * HEAD
    return pl.pallas_call(
        q_kernel,
        grid=(width // block,),
        in_specs=[
            pl.BlockSpec((rows, d), lambda i: (0, 0)),
            pl.BlockSpec((d, block), lambda i: (0, i)),
            pl.BlockSpec((1, block), lambda i: (0, i)),
            pl.BlockSpec((rows, HEAD), lambda i: (0, 0)),
            pl.BlockSpec((rows, HEAD), lambda i: (0, 0)),
        ],
        out_specs=[pl.BlockSpec((rows, block), lambda i: (0, i)), pl.BlockSpec((rows, far), lambda i: (0, 0))],
        out_shape=[jax.ShapeDtypeStruct((rows, width), BF), jax.ShapeDtypeStruct((rows, far), BF)],
        compiler_params=pltpu.CompilerParams(dimension_semantics=("arbitrary",), vmem_limit_bytes=Q_VMEM),
        cost_estimate=pl.CostEstimate(flops=2 * rows * d * width, bytes_accessed=2 * d * width, transcendentals=0),
        name="q_proj",
    )(h, w_qkv, b, cos, sin)


HEADS = 16
MOVED = 3


def given(cp):
    return jnp.where(cp == 3, MOVED, jnp.where(cp == 2, 1, 0))


def taken(cp):
    return given(3 - cp)


STRIP = 256
CHUNK = 256


def attn_kernel(cp_ref, *refs, old, slots, first, far, far_first, backs):
    refs = list(refs)
    take = lambda n: [refs.pop(0) for _ in range(n)]
    far_q = take(2 if far else 0)
    own_q = take(2 if slots else 0)
    k_ref, vt_ref = take(2)
    back_refs = take(backs)
    far_outs = take(1 if far else 0)
    own_outs = take(1 if slots else 0)
    s_ref, p_ref, acc_ref, mx_ref, m_ref, l_ref, al_ref = take(7)
    slot = pl.program_id(0)
    if far and slots:
        q_ref, qn_ref = take(2)
        for at, ref, pair in ((slot, q_ref, (far_q[0], own_q[0])), (slot + 1, qn_ref, (far_q[1], own_q[1]))):
            for is_far, source in ((at < far, pair[0]), (at >= far, pair[1])):
                @pl.when(is_far)
                def _(ref=ref, source=source):
                    ref[...] = source[...]
    else:
        q_ref, qn_ref = far_q or own_q

    rows = q_ref.shape[0]
    strips = rows // STRIP
    chunks = rows // CHUNK
    cp = cp_ref[0]

    def owner_of(slot):
        other = jnp.where(far_first + slot < taken(cp), 3 - cp, -1)
        mine = jnp.where(first + slot - far < HEADS - given(cp), cp, -1)
        return jnp.where(slot < far, other, mine)

    owner = owner_of(slot)
    fresh = (slot == 0) | (owner_of(slot - 1) < 0)

    def scores(qr, base, u, w):
        k = k_ref[pl.ds(base + u * CHUNK, CHUNK), :]
        return lax.dot_general(k, qr[pl.ds(w * STRIP, STRIP), :], (((1,), (1,)), ((), ())), preferred_element_type=F32)

    def col_max(s):
        return s.reshape(CHUNK // 8, 8, STRIP).max(axis=0)

    def triangle(s):
        key = lax.broadcasted_iota(jnp.int32, s.shape, 0)
        query = lax.broadcasted_iota(jnp.int32, s.shape, 1)
        return jnp.where(key <= query, s, NEG)

    def product(base, u, w):
        at = base // HEAD + u * (CHUNK // HEAD)
        vt = jnp.concatenate([vt_ref[at + i] for i in range(CHUNK // HEAD)], axis=1)
        p = jnp.concatenate([p_ref[w * (STRIP // HEAD) + i, pl.ds(u * CHUNK, CHUNK), :] for i in range(STRIP // HEAD)], axis=1)
        return jnp.dot(vt, p, preferred_element_type=F32)

    def stage(ex=None, pv=None, qk=None, diagonal=False):
        for w in range(strips):
            ne = ex[w] if ex else 0
            np_ = pv[1][w] if pv else 0
            nq = qk[2][w] if qk else 0
            cs = pl.ds(w * STRIP, STRIP)
            total = None
            top = None
            if ne:
                m_old = m_ref[0:1, cs]
                m_new = jnp.maximum(m_old, mx_ref[:, cs].max(axis=0, keepdims=True))
                alpha = jnp.exp2((m_old - m_new) * SCALE2)
                l8 = l_ref[:, cs] * alpha
            for u in range(chunks):
                ks = pl.ds(u * CHUNK, CHUNK)
                if u < np_:
                    x = product(pv[0], u, w)
                    total = x if total is None else total + x
                if u < ne:
                    e = jnp.exp2((s_ref[ks, cs] - m_new) * SCALE2)
                    l8 = l8 + e.reshape(CHUNK // 8, 8, STRIP).sum(axis=0)
                    e = e.astype(BF)
                    for i in range(STRIP // HEAD):
                        p_ref[w * (STRIP // HEAD) + i, ks, :] = e[:, i * HEAD:(i + 1) * HEAD]
                if u < nq:
                    s = scores(qk[0], qk[1], u, w)
                    if diagonal and u == nq - 1:
                        s = triangle(s)
                    s_ref[ks, cs] = s
                    x = col_max(s)
                    top = x if top is None else jnp.maximum(top, x)
            if np_:
                acc_ref[:, cs] = acc_ref[:, cs] * al_ref[0:1, cs] + total
            if ne:
                m_ref[:, cs] = jnp.broadcast_to(m_new, (8, STRIP))
                al_ref[:, cs] = jnp.broadcast_to(alpha, (8, STRIP))
                l_ref[:, cs] = l8
            if nq:
                mx_ref[:, cs] = top

    full = [chunks] * strips
    upper = [w + 1 for w in range(strips)]

    @pl.when(fresh & (owner >= 0))
    def _():
        stage(qk=(q_ref, 0, full))
        p_ref[...] = jnp.zeros_like(p_ref)
        acc_ref[...] = jnp.zeros_like(acc_ref)

    @pl.when(owner >= 0)
    def _():
        own = pl.multiple_of(old + rows * owner, rows)
        m_ref[...] = jnp.full_like(m_ref, NEG)
        l_ref[...] = jnp.zeros_like(l_ref)
        al_ref[...] = jnp.zeros_like(al_ref)

        def body(j, carry):
            before = pl.multiple_of(jnp.maximum(j - 1, 0) * rows, rows)
            after = pl.multiple_of((j + 1) * rows, rows)
            stage(full, (before, full), (q_ref, after, full))
            return carry

        lax.fori_loop(0, own // rows - 1, body, 0)
        stage(full, (pl.multiple_of(own - 2 * rows, rows), full), (q_ref, own, upper), diagonal=True)
        stage(upper, (pl.multiple_of(own - rows, rows), full), (qn_ref, 0, full))
        stage(pv=(own, upper))
        for w in range(strips):
            cs = pl.ds(w * STRIP, STRIP)
            o = (acc_ref[:, cs] / l_ref[:, cs].sum(axis=0, keepdims=True)).astype(BF).T
            for out, mine in [(out, slot < far) for out in far_outs] + [(out, slot >= far) for out in own_outs]:
                @pl.when(mine)
                def _(out=out, o=o, cs=cs):
                    out[cs, :] = o

    for i, back_ref in enumerate(back_refs):
        @pl.when((owner < 0) & ((slot == pl.num_programs(0) - 1) == (i == 0)))
        def _(back_ref=back_ref):
            own_outs[0][...] = back_ref[...]


def attention(cp, q, q_far, k_all, vt_all, *, slots=0, first=0, far=0, far_first=0, back=()):
    rows = k_all.shape[0] // 8
    keys = k_all.shape[0]
    row_block = lambda index: pl.BlockSpec((rows, HEAD), index)
    far_col = lambda s: MOVED - 1 - far_first - jnp.clip(s, 0, far - 1)
    own_col = lambda s: first + jnp.clip(s - far, 0, slots - 1)
    operands, in_specs, out_specs, out_shape = [], [], [], []
    for count, source, col, out_col in (
        (far, q_far, far_col, lambda s: far - 1 - jnp.clip(s, 0, far - 1)),
        (slots, q, own_col, lambda s: jnp.clip(s - far, 0, slots - 1)),
    ):
        if count:
            operands += [source, source]
            in_specs += [row_block(lambda s, c, col=col: (0, col(s))), row_block(lambda s, c, col=col: (0, col(s + 1)))]
            out_specs.append(row_block(lambda s, c, col=out_col: (0, col(s))))
            out_shape.append(jax.ShapeDtypeStruct((rows, count * HEAD), BF))
    operands += [k_all, vt_all, *back]
    in_specs += [
        pl.BlockSpec((keys, HEAD), lambda s, c: (0, 0)),
        pl.BlockSpec((keys // HEAD, HEAD, HEAD), lambda s, c: (0, 0, 0)),
    ]
    for i in range(len(back)):
        in_specs.append(row_block((lambda s, c: (0, 0)) if i == 0 else (lambda s, c: (0, jnp.clip(s - far - (slots - MOVED), 0, MOVED - 2)))))
    scratch = [
        pltpu.VMEM((rows, rows), F32),
        pltpu.VMEM((rows // HEAD, rows, HEAD), BF),
        pltpu.VMEM((HEAD, rows), F32),
    ] + [pltpu.VMEM((8, rows), F32)] * 4
    if far and slots:
        scratch += [pltpu.VMEM((rows, HEAD), BF)] * 2
    count = far + slots
    return pl.pallas_call(
        functools.partial(attn_kernel, old=keys // 2, slots=slots, first=first, far=far, far_first=far_first, backs=len(back)),
        grid_spec=pltpu.PrefetchScalarGridSpec(
            num_scalar_prefetch=1, grid=(count,), in_specs=in_specs, out_specs=out_specs, scratch_shapes=scratch
        ),
        out_shape=out_shape,
        compiler_params=pltpu.CompilerParams(dimension_semantics=("arbitrary",), vmem_limit_bytes=ATTN_VMEM),
        cost_estimate=pl.CostEstimate(flops=4 * rows * count * HEAD * keys, bytes_accessed=4 * rows * count * HEAD, transcendentals=0),
        name="attention",
    )(cp, *operands)


def gather_kernel(cp_ref, *refs):
    parts, (k_ref, vt_ref) = refs[:-2], refs[-2:]
    rows = k_ref.shape[0]
    for i, part in enumerate(parts):
        @pl.when(pl.program_id(0) == i)
        def _(part=part):
            k_ref[...] = part[pl.ds(0, rows), :]
            for b in range(rows // HEAD):
                vt_ref[b] = part[pl.ds(rows + b * HEAD, HEAD), :].T


def gather(cp, old, new):
    n = len(old)
    rows = old[0].shape[0] // 2
    place = lambda i, c: jnp.where(i < n, c[0] ^ i, n + lax.rem(c[0] + 2 * n - i, n))
    return pl.pallas_call(
        gather_kernel,
        grid_spec=pltpu.PrefetchScalarGridSpec(
            num_scalar_prefetch=1,
            grid=(2 * n,),
            in_specs=[pl.BlockSpec((2 * rows, HEAD), lambda i, c: (0, 0))] * (2 * n),
            out_specs=[
                pl.BlockSpec((rows, HEAD), lambda i, c: (place(i, c), 0)),
                pl.BlockSpec((rows // HEAD, HEAD, HEAD), lambda i, c: (place(i, c), 0, 0)),
            ],
        ),
        out_shape=[
            jax.ShapeDtypeStruct((2 * n * rows, HEAD), BF),
            jax.ShapeDtypeStruct((2 * n * rows // HEAD, HEAD, HEAD), BF),
        ],
        compiler_params=pltpu.CompilerParams(dimension_semantics=("arbitrary",), vmem_limit_bytes=ATTN_VMEM),
        cost_estimate=pl.CostEstimate(flops=2 ** 20, bytes_accessed=2 ** 23, transcendentals=0),
        name="gather",
    )(cp, *old, *new)


def own_kernel(x_ref, *rest):
    o_refs, w_ref, y_ref = rest[:-2], rest[-2], rest[-1]
    for r in range(x_ref.shape[0] // 256):
        rs = pl.ds(r * 256, 256)
        o = jnp.concatenate([o_ref[rs, :] for o_ref in o_refs], axis=1)
        y_ref[rs, :] = x_ref[rs, :].astype(F32) + jnp.dot(o, w_ref[...], preferred_element_type=F32)


def own_part(x, o_parts, w, block=512):
    rows, d = x.shape
    depth = w.shape[0]
    col = lambda i: (0, i)
    return pl.pallas_call(
        own_kernel,
        grid=(d // block,),
        in_specs=[pl.BlockSpec((rows, block), col)]
        + [pl.BlockSpec(o.shape, lambda i: (0, 0)) for o in o_parts]
        + [pl.BlockSpec((depth, block), col)],
        out_specs=pl.BlockSpec((rows, block), col),
        out_shape=jax.ShapeDtypeStruct((rows, d), F32),
        compiler_params=pltpu.CompilerParams(dimension_semantics=("arbitrary",), vmem_limit_bytes=OUT_VMEM),
        cost_estimate=pl.CostEstimate(flops=2 * rows * d * depth, bytes_accessed=6 * rows * d, transcendentals=0),
        name="own_part",
    )(x, *o_parts, w)


def other_kernel(cp_ref, y_ref, *rest, parts):
    o_refs, w_refs, out_ref, o_buf = rest[:parts], rest[parts:-2], rest[-2], rest[-1]

    @pl.when(pl.program_id(0) == 0)
    def _():
        at = 0
        for o_ref in o_refs:
            o_buf[:, pl.ds(at, o_ref.shape[1])] = o_ref[...]
            at += o_ref.shape[1]

    pieces = len(w_refs) // 4
    depth = sum(w_ref.shape[0] for w_ref in w_refs[:pieces])
    for r in range(y_ref.shape[0] // 256):
        rs = pl.ds(r * 256, 256)
        total = None
        for i in range(4):
            at = pl.multiple_of((cp_ref[0] ^ i) * depth, depth)
            w = jnp.concatenate([w_ref[...] for w_ref in w_refs[i * pieces:(i + 1) * pieces]], axis=0)
            x = jnp.dot(o_buf[rs, pl.ds(at, depth)], w, preferred_element_type=F32)
            total = x if total is None else total + x
        out_ref[rs, :] = (y_ref[rs, :] + total).astype(BF)


def other_part(cp, y, o_parts, w_parts, block=512):
    rows, d = y.shape
    col = lambda i, c: (0, i)
    depth = sum(w.shape[0] for w in w_parts)
    return pl.pallas_call(
        functools.partial(other_kernel, parts=len(o_parts)),
        grid_spec=pltpu.PrefetchScalarGridSpec(
            num_scalar_prefetch=1,
            grid=(d // block,),
            in_specs=[pl.BlockSpec((rows, block), col)]
            + [pl.BlockSpec(o.shape, lambda i, c: (0, 0)) for o in o_parts]
            + [pl.BlockSpec((w.shape[0], block), col) for w in w_parts],
            out_specs=pl.BlockSpec((rows, block), col),
            scratch_shapes=[pltpu.VMEM((rows, depth), BF)],
        ),
        out_shape=jax.ShapeDtypeStruct((rows, d), BF),
        compiler_params=pltpu.CompilerParams(dimension_semantics=("arbitrary",), vmem_limit_bytes=OUT_VMEM),
        cost_estimate=pl.CostEstimate(flops=2 * rows * d * depth, bytes_accessed=6 * rows * d, transcendentals=0),
        name="other_part",
    )(cp, y, *o_parts, *w_parts)


SIZES = (4, 5, 3, 4)
PIECE_ROWS = (128, 384)
PIECES = len(PIECE_ROWS)


def after(a, *others):
    return lax.optimization_barrier((a, *others))[0]


def local_step(x, k_cache, v_cache, rope_table, norm_gain, w_qkv, b_qkv, w_out):
    rows = x.shape[0]
    n = lax.axis_size("cp")
    cp = lax.axis_index("cp")
    swap = [(0, 1), (1, 0)]
    width = w_out.shape[0]
    quarter = width // n
    where = cp.astype(jnp.int32)[None]
    around = lambda s: [(i, (i + s) % n) for i in range(n)]
    flip = lambda bits: [(i, i ^ bits) for i in range(n)]

    kv_cache = jnp.concatenate([k_cache[:, 0], v_cache[:, 0]], axis=0)
    old = [kv_cache, lax.ppermute(kv_cache, "cp", flip(1)), lax.ppermute(kv_cache, "cp", flip(2))]
    mine = lax.dynamic_slice_in_dim(w_out, cp * quarter, PIECE_ROWS[0], 0)
    w_peer = [lax.ppermute(mine, "tp", swap)]

    bias = b_qkv[None]
    h, kv_new, new_k, new_v, cos, sin, mine = norm_kv(where, x, norm_gain[None], w_qkv, bias, rope_table, w_out)
    w_peer.append(lax.ppermute(mine, "tp", swap))
    old.append(lax.ppermute(after(old[2], kv_new), "cp", flip(1)))
    kv_new = kv_new.reshape(2 * rows, HEAD)
    new = [kv_new] + [lax.ppermute(kv_new, "cp", around(s)) for s in range(1, n)]
    queries, q_far = q_proj(h, w_qkv, bias, cos, sin, width)
    q_far = lax.ppermute(q_far, "cp", [(3, 0), (2, 1)])
    w_peer[0] = after(w_peer[0], queries)

    k_all, vt_all = gather(where, old, new)
    attend = functools.partial(attention, where, k_all=k_all, vt_all=vt_all)

    o_own, o_other = [], []
    w_x, w_core, w_far = [None] * PIECES, [None] * PIECES, [None] * PIECES

    def heads(i, *previous, far=0, far_first=0, back=()):
        q = after(queries, *previous) if previous else queries
        outs = attend(q, q_far, slots=SIZES[i], first=sum(SIZES[:i]), far=far, far_first=far_first, back=back)
        o_own.append(outs[-1])
        o_other.append(lax.ppermute(outs[-1], "tp", swap))
        return outs

    def spread(i):
        w_x[i] = lax.ppermute(w_peer[i], "cp", flip(2))
        w_core[i] = lax.ppermute(w_peer[i], "cp", flip(1))

    def spread_on(i):
        w_far[i] = lax.ppermute(w_x[i], "cp", flip(1))

    spread(0)
    (part,) = heads(0)
    (far,) = attend(None, after(q_far, part), far=1)
    back0 = lax.ppermute(far, "cp", [(0, 3), (1, 2)])
    w_peer[1] = after(w_peer[1], far)
    spread(1)
    far, part = heads(1, far, far=MOVED - 1, far_first=1)
    back1 = lax.ppermute(far, "cp", [(0, 3)])
    (part,) = heads(2, part)
    (part,) = heads(3, part, back=(back0, back1))
    w_x = [after(w, part) for w in w_x]
    spread_on(0)
    spread_on(1)

    y = own_part(x, o_own, w_out)
    y = other_part(where, y, o_other, [*w_peer, *w_core, *w_x, *w_far])
    return y, new_k[:, None], new_v[:, None]


def solution(mesh):
    row_spec = P(("dp", "cp"), None)
    cache_spec = P(("dp", "cp"), "tp", None)
    return jax.shard_map(
        local_step,
        mesh=mesh,
        in_specs=(row_spec, cache_spec, cache_spec, row_spec, P(None), P(None, "tp"), P("tp"), P("tp", None)),
        out_specs=(row_spec, cache_spec, cache_spec),
        check_vma=False,
    )
```

```python
import functools
import math

import jax
import jax.numpy as jnp
from jax import lax
from jax.experimental import pallas as pl
from jax.experimental.pallas import tpu as pltpu
from jax.sharding import PartitionSpec as P


EPS = 1.5625e-07
NEG = -1e30
HEAD = 128
SCALE2 = HEAD ** -0.5 * math.log2(math.e)
F32 = jnp.float32
BF = jnp.bfloat16
ATTN_VMEM = 24 * 2 ** 20
NORM_VMEM = 36 * 2 ** 20
Q_VMEM = 36 * 2 ** 20
OUT_VMEM = 28 * 2 ** 20


def rotate(a, cos, sin):
    lane = lax.broadcasted_iota(jnp.int32, a.shape, 1)
    other = jnp.where(lane % 2 == 0, pltpu.roll(a, HEAD - 1, 1), pltpu.roll(a, 1, 1))
    return a * cos + other * sin


def norm_kv_kernel(cp_ref, x_ref, g_ref, w_ref, b_ref, table_ref, piece_ref, h_ref, kv_ref, k_ref, v_ref, cos_ref, sin_ref, copy_ref):
    copy_ref[...] = piece_ref[...]
    pairs = table_ref.shape[1] // 2
    lane = lax.broadcasted_iota(jnp.int32, (pairs, HEAD), 1)
    hit = lax.broadcasted_iota(jnp.int32, (pairs, HEAD), 0) == lane // 2
    spread = functools.partial(jnp.dot, precision=lax.Precision.HIGHEST, preferred_element_type=F32)
    stay = lax.broadcasted_iota(jnp.int32, (128, HEAD), 1) >= 2 * pairs
    for r in range(x_ref.shape[0] // 128):
        rs = pl.ds(r * 128, 128)
        table = table_ref[rs, :]
        cos = jnp.where(stay, 1.0, spread(table[:, :pairs], hit.astype(F32)))
        sin = spread(table[:, pairs:], jnp.where(hit, jnp.where(lane % 2 == 0, -1.0, 1.0), 0.0))
        cos_ref[rs, :] = cos
        sin_ref[rs, :] = sin
        x = x_ref[rs, :].astype(F32)
        inv = lax.rsqrt(jnp.mean(x * x, axis=-1, keepdims=True) + EPS)
        h = (x * inv * g_ref[...].astype(F32)).astype(BF)
        h_ref[rs, :] = h
        a = jnp.dot(h, w_ref[...], preferred_element_type=F32) + b_ref[...].astype(F32)
        k = rotate(a[:, :HEAD], cos, sin).astype(BF)
        v = a[:, HEAD:].astype(BF)
        k_ref[rs, :] = k
        v_ref[rs, :] = v
        kv_ref[0, rs, :] = k
        kv_ref[1, rs, :] = v


def norm_kv(cp, x, g, w_qkv, b, table, w_out, block=256):
    rows, d = x.shape
    steps = rows // block
    last = w_qkv.shape[1] // (2 * HEAD) - 1
    row = lambda i, c: (i, 0)
    skip, piece = PIECE_ROWS
    pieces = piece // skip
    copied = lambda i: jnp.minimum(i, pieces - 1)
    head_rows = pl.BlockSpec((block, HEAD), row)
    return pl.pallas_call(
        norm_kv_kernel,
        grid_spec=pltpu.PrefetchScalarGridSpec(
            num_scalar_prefetch=1,
            grid=(steps,),
            in_specs=[
                pl.BlockSpec((block, d), row),
                pl.BlockSpec((1, d), lambda i, c: (0, 0)),
                pl.BlockSpec((d, 2 * HEAD), lambda i, c: (0, last)),
                pl.BlockSpec((1, 2 * HEAD), lambda i, c: (0, last)),
                pl.BlockSpec((block, table.shape[1]), row),
                pl.BlockSpec((skip, w_out.shape[1]), lambda i, c: (c[0] * (pieces + 1) + 1 + copied(i), 0)),
            ],
            out_specs=[
                pl.BlockSpec((block, d), row),
                pl.BlockSpec((2, block, HEAD), lambda i, c: (0, i, 0)),
                head_rows,
                head_rows,
                head_rows,
                head_rows,
                pl.BlockSpec((skip, w_out.shape[1]), lambda i, c: (copied(i), 0)),
            ],
        ),
        out_shape=[
            jax.ShapeDtypeStruct((rows, d), BF),
            jax.ShapeDtypeStruct((2, rows, HEAD), BF),
            jax.ShapeDtypeStruct((rows, HEAD), BF),
            jax.ShapeDtypeStruct((rows, HEAD), BF),
            jax.ShapeDtypeStruct((rows, HEAD), F32),
            jax.ShapeDtypeStruct((rows, HEAD), F32),
            jax.ShapeDtypeStruct((piece, w_out.shape[1]), BF),
        ],
        compiler_params=pltpu.CompilerParams(dimension_semantics=("arbitrary",), vmem_limit_bytes=NORM_VMEM),
        cost_estimate=pl.CostEstimate(flops=2 * rows * d * 2 * HEAD, bytes_accessed=4 * rows * d, transcendentals=0),
        name="norm_kv",
    )(cp, x, g, w_qkv, b, table, w_out)


def q_kernel(h_ref, w_ref, b_ref, cos_ref, sin_ref, q_ref, far_ref):
    lead = far_ref.shape[1] - w_ref.shape[1]
    for r in range(h_ref.shape[0] // 128):
        rs = pl.ds(r * 128, 128)
        a = jnp.dot(h_ref[rs, :], w_ref[...], preferred_element_type=F32) + b_ref[...].astype(F32)
        for i in range(a.shape[1] // HEAD):
            at = slice(i * HEAD, (i + 1) * HEAD)
            q = rotate(a[:, at], cos_ref[rs, :], sin_ref[rs, :]).astype(BF)
            q_ref[rs, at] = q
            if i * HEAD + lead >= 0:
                far_ref[rs, pl.ds(i * HEAD + lead, HEAD)] = q


def q_proj(h, w_qkv, b, cos, sin, width, block=512):
    rows, d = h.shape
    far = MOVED * HEAD
    return pl.pallas_call(
        q_kernel,
        grid=(width // block,),
        in_specs=[
            pl.BlockSpec((rows, d), lambda i: (0, 0)),
            pl.BlockSpec((d, block), lambda i: (0, i)),
            pl.BlockSpec((1, block), lambda i: (0, i)),
            pl.BlockSpec((rows, HEAD), lambda i: (0, 0)),
            pl.BlockSpec((rows, HEAD), lambda i: (0, 0)),
        ],
        out_specs=[pl.BlockSpec((rows, block), lambda i: (0, i)), pl.BlockSpec((rows, far), lambda i: (0, 0))],
        out_shape=[jax.ShapeDtypeStruct((rows, width), BF), jax.ShapeDtypeStruct((rows, far), BF)],
        compiler_params=pltpu.CompilerParams(dimension_semantics=("arbitrary",), vmem_limit_bytes=Q_VMEM),
        cost_estimate=pl.CostEstimate(flops=2 * rows * d * width, bytes_accessed=2 * d * width, transcendentals=0),
        name="q_proj",
    )(h, w_qkv, b, cos, sin)


HEADS = 16
MOVED = 3


def given(cp):
    return jnp.where(cp == 3, MOVED, jnp.where(cp == 2, 1, 0))


def taken(cp):
    return given(3 - cp)


STRIP = 256
CHUNK = 256


def attn_kernel(cp_ref, *refs, old, slots, first, far, far_first, backs):
    refs = list(refs)
    take = lambda n: [refs.pop(0) for _ in range(n)]
    far_q = take(2 if far else 0)
    own_q = take(2 if slots else 0)
    k_ref, vt_ref = take(2)
    back_refs = take(backs)
    far_outs = take(1 if far else 0)
    own_outs = take(1 if slots else 0)
    s_ref, p_ref, acc_ref, mx_ref, m_ref, l_ref, al_ref = take(7)
    slot = pl.program_id(0)
    if far and slots:
        q_ref, qn_ref = take(2)
        for at, ref, pair in ((slot, q_ref, (far_q[0], own_q[0])), (slot + 1, qn_ref, (far_q[1], own_q[1]))):
            for is_far, source in ((at < far, pair[0]), (at >= far, pair[1])):
                @pl.when(is_far)
                def _(ref=ref, source=source):
                    ref[...] = source[...]
    else:
        q_ref, qn_ref = far_q or own_q

    rows = q_ref.shape[0]
    strips = rows // STRIP
    chunks = rows // CHUNK
    cp = cp_ref[0]

    def owner_of(slot):
        other = jnp.where(far_first + slot < taken(cp), 3 - cp, -1)
        mine = jnp.where(first + slot - far < HEADS - given(cp), cp, -1)
        return jnp.where(slot < far, other, mine)

    owner = owner_of(slot)
    fresh = (slot == 0) | (owner_of(slot - 1) < 0)

    def scores(qr, base, u, w):
        k = k_ref[pl.ds(base + u * CHUNK, CHUNK), :]
        return lax.dot_general(k, qr[pl.ds(w * STRIP, STRIP), :], (((1,), (1,)), ((), ())), preferred_element_type=F32)

    def col_max(s):
        return s.reshape(CHUNK // 8, 8, STRIP).max(axis=0)

    def triangle(s):
        key = lax.broadcasted_iota(jnp.int32, s.shape, 0)
        query = lax.broadcasted_iota(jnp.int32, s.shape, 1)
        return jnp.where(key <= query, s, NEG)

    def product(base, u, w):
        at = base // HEAD + u * (CHUNK // HEAD)
        vt = jnp.concatenate([vt_ref[at + i] for i in range(CHUNK // HEAD)], axis=1)
        p = jnp.concatenate([p_ref[w * (STRIP // HEAD) + i, pl.ds(u * CHUNK, CHUNK), :] for i in range(STRIP // HEAD)], axis=1)
        return jnp.dot(vt, p, preferred_element_type=F32)

    def stage(ex=None, pv=None, qk=None, diagonal=False):
        for w in range(strips):
            ne = ex[w] if ex else 0
            np_ = pv[1][w] if pv else 0
            nq = qk[2][w] if qk else 0
            cs = pl.ds(w * STRIP, STRIP)
            total = None
            top = None
            if ne:
                m_old = m_ref[0:1, cs]
                m_new = jnp.maximum(m_old, mx_ref[:, cs].max(axis=0, keepdims=True))
                alpha = jnp.exp2((m_old - m_new) * SCALE2)
                l8 = l_ref[:, cs] * alpha
            for u in range(chunks):
                ks = pl.ds(u * CHUNK, CHUNK)
                if u < np_:
                    x = product(pv[0], u, w)
                    total = x if total is None else total + x
                if u < ne:
                    e = jnp.exp2((s_ref[ks, cs] - m_new) * SCALE2)
                    l8 = l8 + e.reshape(CHUNK // 8, 8, STRIP).sum(axis=0)
                    e = e.astype(BF)
                    for i in range(STRIP // HEAD):
                        p_ref[w * (STRIP // HEAD) + i, ks, :] = e[:, i * HEAD:(i + 1) * HEAD]
                if u < nq:
                    s = scores(qk[0], qk[1], u, w)
                    if diagonal and u == nq - 1:
                        s = triangle(s)
                    s_ref[ks, cs] = s
                    x = col_max(s)
                    top = x if top is None else jnp.maximum(top, x)
            if np_:
                acc_ref[:, cs] = acc_ref[:, cs] * al_ref[0:1, cs] + total
            if ne:
                m_ref[:, cs] = jnp.broadcast_to(m_new, (8, STRIP))
                al_ref[:, cs] = jnp.broadcast_to(alpha, (8, STRIP))
                l_ref[:, cs] = l8
            if nq:
                mx_ref[:, cs] = top

    full = [chunks] * strips
    upper = [w + 1 for w in range(strips)]

    @pl.when(fresh & (owner >= 0))
    def _():
        stage(qk=(q_ref, 0, full))
        p_ref[...] = jnp.zeros_like(p_ref)
        acc_ref[...] = jnp.zeros_like(acc_ref)

    @pl.when(owner >= 0)
    def _():
        own = pl.multiple_of(old + rows * owner, rows)
        m_ref[...] = jnp.full_like(m_ref, NEG)
        l_ref[...] = jnp.zeros_like(l_ref)
        al_ref[...] = jnp.zeros_like(al_ref)

        def body(j, carry):
            before = pl.multiple_of(jnp.maximum(j - 1, 0) * rows, rows)
            after = pl.multiple_of((j + 1) * rows, rows)
            stage(full, (before, full), (q_ref, after, full))
            return carry

        lax.fori_loop(0, own // rows - 1, body, 0)
        stage(full, (pl.multiple_of(own - 2 * rows, rows), full), (q_ref, own, upper), diagonal=True)
        stage(upper, (pl.multiple_of(own - rows, rows), full), (qn_ref, 0, full))
        stage(pv=(own, upper))
        outs = []
        for w in range(strips):
            cs = pl.ds(w * STRIP, STRIP)
            outs.append((acc_ref[:, cs] / l_ref[:, cs].sum(axis=0, keepdims=True)).astype(BF).T)

        def write(out):
            for w in range(strips):
                out[pl.ds(w * STRIP, STRIP), :] = outs[w]

        if far and slots:
            pl.when(slot < far)(functools.partial(write, far_outs[0]))
            pl.when(slot >= far)(functools.partial(write, own_outs[0]))
        else:
            write((far_outs + own_outs)[0])

    for i, back_ref in enumerate(back_refs):
        @pl.when((owner < 0) & ((slot == pl.num_programs(0) - 1) == (i == 0)))
        def _(back_ref=back_ref):
            own_outs[0][...] = back_ref[...]


def attention(cp, q, q_far, k_all, vt_all, *, slots=0, first=0, far=0, far_first=0, back=()):
    rows = k_all.shape[0] // 8
    keys = k_all.shape[0]
    row_block = lambda index: pl.BlockSpec((rows, HEAD), index)
    far_col = lambda s: MOVED - 1 - far_first - jnp.clip(s, 0, far - 1)
    own_col = lambda s: first + jnp.clip(s - far, 0, slots - 1)
    operands, in_specs, out_specs, out_shape = [], [], [], []
    for count, source, col, out_col in (
        (far, q_far, far_col, lambda s: far - 1 - jnp.clip(s, 0, far - 1)),
        (slots, q, own_col, lambda s: jnp.clip(s - far, 0, slots - 1)),
    ):
        if count:
            operands += [source, source]
            in_specs += [row_block(lambda s, c, col=col: (0, col(s))), row_block(lambda s, c, col=col: (0, col(s + 1)))]
            out_specs.append(row_block(lambda s, c, col=out_col: (0, col(s))))
            out_shape.append(jax.ShapeDtypeStruct((rows, count * HEAD), BF))
    operands += [k_all, vt_all, *back]
    in_specs += [
        pl.BlockSpec((keys, HEAD), lambda s, c: (0, 0)),
        pl.BlockSpec((keys // HEAD, HEAD, HEAD), lambda s, c: (0, 0, 0)),
    ]
    for i in range(len(back)):
        in_specs.append(row_block((lambda s, c: (0, 0)) if i == 0 else (lambda s, c: (0, jnp.clip(s - far - (slots - MOVED), 0, MOVED - 2)))))
    scratch = [
        pltpu.VMEM((rows, rows), F32),
        pltpu.VMEM((rows // HEAD, rows, HEAD), BF),
        pltpu.VMEM((HEAD, rows), F32),
    ] + [pltpu.VMEM((8, rows), F32)] * 4
    if far and slots:
        scratch += [pltpu.VMEM((rows, HEAD), BF)] * 2
    count = far + slots
    return pl.pallas_call(
        functools.partial(attn_kernel, old=keys // 2, slots=slots, first=first, far=far, far_first=far_first, backs=len(back)),
        grid_spec=pltpu.PrefetchScalarGridSpec(
            num_scalar_prefetch=1, grid=(count,), in_specs=in_specs, out_specs=out_specs, scratch_shapes=scratch
        ),
        out_shape=out_shape,
        compiler_params=pltpu.CompilerParams(dimension_semantics=("arbitrary",), vmem_limit_bytes=ATTN_VMEM),
        cost_estimate=pl.CostEstimate(flops=4 * rows * count * HEAD * keys, bytes_accessed=4 * rows * count * HEAD, transcendentals=0),
        name="attention",
    )(cp, *operands)


def gather_kernel(cp_ref, *refs):
    parts, (k_ref, vt_ref) = refs[:-2], refs[-2:]
    rows = k_ref.shape[0]
    for i, part in enumerate(parts):
        @pl.when(pl.program_id(0) == i)
        def _(part=part):
            k_ref[...] = part[pl.ds(0, rows), :]
            for b in range(rows // HEAD):
                vt_ref[b] = part[pl.ds(rows + b * HEAD, HEAD), :].T


def gather(cp, old, new):
    n = len(old)
    rows = old[0].shape[0] // 2
    place = lambda i, c: jnp.where(i < n, c[0] ^ i, n + lax.rem(c[0] + 2 * n - i, n))
    return pl.pallas_call(
        gather_kernel,
        grid_spec=pltpu.PrefetchScalarGridSpec(
            num_scalar_prefetch=1,
            grid=(2 * n,),
            in_specs=[pl.BlockSpec((2 * rows, HEAD), lambda i, c: (0, 0))] * (2 * n),
            out_specs=[
                pl.BlockSpec((rows, HEAD), lambda i, c: (place(i, c), 0)),
                pl.BlockSpec((rows // HEAD, HEAD, HEAD), lambda i, c: (place(i, c), 0, 0)),
            ],
        ),
        out_shape=[
            jax.ShapeDtypeStruct((2 * n * rows, HEAD), BF),
            jax.ShapeDtypeStruct((2 * n * rows // HEAD, HEAD, HEAD), BF),
        ],
        compiler_params=pltpu.CompilerParams(dimension_semantics=("arbitrary",), vmem_limit_bytes=ATTN_VMEM),
        cost_estimate=pl.CostEstimate(flops=2 ** 20, bytes_accessed=2 ** 23, transcendentals=0),
        name="gather",
    )(cp, *old, *new)


def own_kernel(x_ref, *rest):
    o_refs, w_ref, y_ref = rest[:-2], rest[-2], rest[-1]
    for r in range(x_ref.shape[0] // 256):
        rs = pl.ds(r * 256, 256)
        o = jnp.concatenate([o_ref[rs, :] for o_ref in o_refs], axis=1)
        y_ref[rs, :] = x_ref[rs, :].astype(F32) + jnp.dot(o, w_ref[...], preferred_element_type=F32)


def own_part(x, o_parts, w, block=512):
    rows, d = x.shape
    depth = w.shape[0]
    col = lambda i: (0, i)
    return pl.pallas_call(
        own_kernel,
        grid=(d // block,),
        in_specs=[pl.BlockSpec((rows, block), col)]
        + [pl.BlockSpec(o.shape, lambda i: (0, 0)) for o in o_parts]
        + [pl.BlockSpec((depth, block), col)],
        out_specs=pl.BlockSpec((rows, block), col),
        out_shape=jax.ShapeDtypeStruct((rows, d), F32),
        compiler_params=pltpu.CompilerParams(dimension_semantics=("arbitrary",), vmem_limit_bytes=OUT_VMEM),
        cost_estimate=pl.CostEstimate(flops=2 * rows * d * depth, bytes_accessed=6 * rows * d, transcendentals=0),
        name="own_part",
    )(x, *o_parts, w)


def other_kernel(cp_ref, y_ref, *rest, parts):
    o_refs, w_refs, out_ref, o_buf = rest[:parts], rest[parts:-2], rest[-2], rest[-1]

    @pl.when(pl.program_id(0) == 0)
    def _():
        at = 0
        for o_ref in o_refs:
            o_buf[:, pl.ds(at, o_ref.shape[1])] = o_ref[...]
            at += o_ref.shape[1]

    pieces = len(w_refs) // 4
    depth = sum(w_ref.shape[0] for w_ref in w_refs[:pieces])
    for r in range(y_ref.shape[0] // 256):
        rs = pl.ds(r * 256, 256)
        total = None
        for i in range(4):
            at = pl.multiple_of((cp_ref[0] ^ i) * depth, depth)
            w = jnp.concatenate([w_ref[...] for w_ref in w_refs[i * pieces:(i + 1) * pieces]], axis=0)
            x = jnp.dot(o_buf[rs, pl.ds(at, depth)], w, preferred_element_type=F32)
            total = x if total is None else total + x
        out_ref[rs, :] = (y_ref[rs, :] + total).astype(BF)


def other_part(cp, y, o_parts, w_parts, block=512):
    rows, d = y.shape
    col = lambda i, c: (0, i)
    depth = sum(w.shape[0] for w in w_parts)
    return pl.pallas_call(
        functools.partial(other_kernel, parts=len(o_parts)),
        grid_spec=pltpu.PrefetchScalarGridSpec(
            num_scalar_prefetch=1,
            grid=(d // block,),
            in_specs=[pl.BlockSpec((rows, block), col)]
            + [pl.BlockSpec(o.shape, lambda i, c: (0, 0)) for o in o_parts]
            + [pl.BlockSpec((w.shape[0], block), col) for w in w_parts],
            out_specs=pl.BlockSpec((rows, block), col),
            scratch_shapes=[pltpu.VMEM((rows, depth), BF)],
        ),
        out_shape=jax.ShapeDtypeStruct((rows, d), BF),
        compiler_params=pltpu.CompilerParams(dimension_semantics=("arbitrary",), vmem_limit_bytes=OUT_VMEM),
        cost_estimate=pl.CostEstimate(flops=2 * rows * d * depth, bytes_accessed=6 * rows * d, transcendentals=0),
        name="other_part",
    )(cp, y, *o_parts, *w_parts)


SIZES = (5, 4, 3, 4)
PIECE_ROWS = (128, 384)
PIECES = len(PIECE_ROWS)


def after(a, *others):
    return lax.optimization_barrier((a, *others))[0]


def local_step(x, k_cache, v_cache, rope_table, norm_gain, w_qkv, b_qkv, w_out):
    rows = x.shape[0]
    n = lax.axis_size("cp")
    cp = lax.axis_index("cp")
    swap = [(0, 1), (1, 0)]
    width = w_out.shape[0]
    quarter = width // n
    where = cp.astype(jnp.int32)[None]
    around = lambda s: [(i, (i + s) % n) for i in range(n)]
    flip = lambda bits: [(i, i ^ bits) for i in range(n)]

    kv_cache = jnp.concatenate([k_cache[:, 0], v_cache[:, 0]], axis=0)
    old = [kv_cache, lax.ppermute(kv_cache, "cp", flip(1)), lax.ppermute(kv_cache, "cp", flip(2))]
    mine = lax.dynamic_slice_in_dim(w_out, cp * quarter, PIECE_ROWS[0], 0)
    w_peer = [lax.ppermute(mine, "tp", swap)]

    bias = b_qkv[None]
    h, kv_new, new_k, new_v, cos, sin, mine = norm_kv(where, x, norm_gain[None], w_qkv, bias, rope_table, w_out)
    w_peer.append(lax.ppermute(mine, "tp", swap))
    old.append(lax.ppermute(after(old[2], kv_new), "cp", flip(1)))
    kv_new = kv_new.reshape(2 * rows, HEAD)
    new = [kv_new] + [lax.ppermute(kv_new, "cp", around(s)) for s in range(1, n)]
    queries, q_far = q_proj(h, w_qkv, bias, cos, sin, width)
    q_far = lax.ppermute(q_far, "cp", [(3, 0), (2, 1)])
    w_peer[0] = after(w_peer[0], queries)

    k_all, vt_all = gather(where, old, new)
    attend = functools.partial(attention, where, k_all=k_all, vt_all=vt_all)

    o_own, o_other = [], []
    w_x, w_core, w_far = [None] * PIECES, [None] * PIECES, [None] * PIECES

    def heads(i, *previous, far=0, far_first=0, back=()):
        q = after(queries, *previous) if previous else queries
        outs = attend(q, q_far, slots=SIZES[i], first=sum(SIZES[:i]), far=far, far_first=far_first, back=back)
        o_own.append(outs[-1])
        o_other.append(lax.ppermute(outs[-1], "tp", swap))
        return outs

    def spread(i):
        w_x[i] = lax.ppermute(w_peer[i], "cp", flip(2))
        w_core[i] = lax.ppermute(w_peer[i], "cp", flip(1))

    def spread_on(i):
        w_far[i] = lax.ppermute(w_x[i], "cp", flip(1))

    spread(0)
    (part,) = heads(0)
    (far,) = attend(None, after(q_far, part), far=1)
    back0 = lax.ppermute(far, "cp", [(0, 3), (1, 2)])
    w_peer[1] = after(w_peer[1], far)
    spread(1)
    far, part = heads(1, far, far=MOVED - 1, far_first=1)
    back1 = lax.ppermute(far, "cp", [(0, 3)])
    (part,) = heads(2, part)
    (part,) = heads(3, part, back=(back0, back1))
    w_x = [after(w, part) for w in w_x]
    spread_on(0)
    spread_on(1)

    y = own_part(x, o_own, w_out)
    y = other_part(where, y, o_other, [*w_peer, *w_core, *w_x, *w_far])
    return y, new_k[:, None], new_v[:, None]


def solution(mesh):
    row_spec = P(("dp", "cp"), None)
    cache_spec = P(("dp", "cp"), "tp", None)
    return jax.shard_map(
        local_step,
        mesh=mesh,
        in_specs=(row_spec, cache_spec, cache_spec, row_spec, P(None), P(None, "tp"), P("tp"), P("tp", None)),
        out_specs=(row_spec, cache_spec, cache_spec),
        check_vma=False,
    )
```

```python
import functools
import math

import jax
import jax.numpy as jnp
from jax import lax
from jax.experimental import pallas as pl
from jax.experimental.pallas import tpu as pltpu
from jax.sharding import PartitionSpec as P


EPS = 1.5625e-07
NEG = -1e30
HEAD = 128
SCALE2 = HEAD ** -0.5 * math.log2(math.e)
F32 = jnp.float32
BF = jnp.bfloat16
ATTN_VMEM = 24 * 2 ** 20
NORM_VMEM = 36 * 2 ** 20
Q_VMEM = 36 * 2 ** 20
OUT_VMEM = 28 * 2 ** 20
OTHER_VMEM = 58 * 2 ** 20


def rotate(a, cos, sin):
    lane = lax.broadcasted_iota(jnp.int32, a.shape, 1)
    other = jnp.where(lane % 2 == 0, pltpu.roll(a, HEAD - 1, 1), pltpu.roll(a, 1, 1))
    return a * cos + other * sin


def norm_kv_kernel(cp_ref, x_ref, g_ref, w_ref, b_ref, table_ref, piece_ref, h_ref, kv_ref, k_ref, v_ref, cos_ref, sin_ref, copy_ref):
    copy_ref[...] = piece_ref[...]
    pairs = table_ref.shape[1] // 2
    lane = lax.broadcasted_iota(jnp.int32, (pairs, HEAD), 1)
    hit = lax.broadcasted_iota(jnp.int32, (pairs, HEAD), 0) == lane // 2
    spread = functools.partial(jnp.dot, precision=lax.Precision.HIGHEST, preferred_element_type=F32)
    stay = lax.broadcasted_iota(jnp.int32, (128, HEAD), 1) >= 2 * pairs
    for r in range(x_ref.shape[0] // 128):
        rs = pl.ds(r * 128, 128)
        table = table_ref[rs, :]
        cos = jnp.where(stay, 1.0, spread(table[:, :pairs], hit.astype(F32)))
        sin = spread(table[:, pairs:], jnp.where(hit, jnp.where(lane % 2 == 0, -1.0, 1.0), 0.0))
        cos_ref[rs, :] = cos
        sin_ref[rs, :] = sin
        x = x_ref[rs, :].astype(F32)
        inv = lax.rsqrt(jnp.mean(x * x, axis=-1, keepdims=True) + EPS)
        h = (x * inv * g_ref[...].astype(F32)).astype(BF)
        h_ref[rs, :] = h
        a = jnp.dot(h, w_ref[...], preferred_element_type=F32) + b_ref[...].astype(F32)
        k = rotate(a[:, :HEAD], cos, sin).astype(BF)
        v = a[:, HEAD:].astype(BF)
        k_ref[rs, :] = k
        v_ref[rs, :] = v
        kv_ref[0, rs, :] = k
        kv_ref[1, rs, :] = v


def norm_kv(cp, x, g, w_qkv, b, table, w_out, block=256):
    rows, d = x.shape
    steps = rows // block
    last = w_qkv.shape[1] // (2 * HEAD) - 1
    row = lambda i, c: (i, 0)
    skip, piece = PIECE_ROWS
    part = piece // steps
    quarter = skip + piece
    head_rows = pl.BlockSpec((block, HEAD), row)
    return pl.pallas_call(
        norm_kv_kernel,
        grid_spec=pltpu.PrefetchScalarGridSpec(
            num_scalar_prefetch=1,
            grid=(steps,),
            in_specs=[
                pl.BlockSpec((block, d), row),
                pl.BlockSpec((1, d), lambda i, c: (0, 0)),
                pl.BlockSpec((d, 2 * HEAD), lambda i, c: (0, last)),
                pl.BlockSpec((1, 2 * HEAD), lambda i, c: (0, last)),
                pl.BlockSpec((block, table.shape[1]), row),
                pl.BlockSpec((pl.Element(part), pl.Element(w_out.shape[1])), lambda i, c: (pl.multiple_of(c[0] * quarter + skip + i * part, 16), 0)),
            ],
            out_specs=[
                pl.BlockSpec((block, d), row),
                pl.BlockSpec((2, block, HEAD), lambda i, c: (0, i, 0)),
                head_rows,
                head_rows,
                head_rows,
                head_rows,
                pl.BlockSpec((part, w_out.shape[1]), row),
            ],
        ),
        out_shape=[
            jax.ShapeDtypeStruct((rows, d), BF),
            jax.ShapeDtypeStruct((2, rows, HEAD), BF),
            jax.ShapeDtypeStruct((rows, HEAD), BF),
            jax.ShapeDtypeStruct((rows, HEAD), BF),
            jax.ShapeDtypeStruct((rows, HEAD), F32),
            jax.ShapeDtypeStruct((rows, HEAD), F32),
            jax.ShapeDtypeStruct((piece, w_out.shape[1]), BF),
        ],
        compiler_params=pltpu.CompilerParams(dimension_semantics=("arbitrary",), vmem_limit_bytes=NORM_VMEM),
        cost_estimate=pl.CostEstimate(flops=2 * rows * d * 2 * HEAD, bytes_accessed=4 * rows * d, transcendentals=0),
        name="norm_kv",
    )(cp, x, g, w_qkv, b, table, w_out)


def q_kernel(h_ref, w_ref, b_ref, cos_ref, sin_ref, q_ref, far_ref):
    lead = far_ref.shape[1] - w_ref.shape[1]
    for r in range(h_ref.shape[0] // 128):
        rs = pl.ds(r * 128, 128)
        a = jnp.dot(h_ref[rs, :], w_ref[...], preferred_element_type=F32) + b_ref[...].astype(F32)
        for i in range(a.shape[1] // HEAD):
            at = slice(i * HEAD, (i + 1) * HEAD)
            q = rotate(a[:, at], cos_ref[rs, :], sin_ref[rs, :]).astype(BF)
            q_ref[rs, at] = q
            if i * HEAD + lead >= 0:
                far_ref[rs, pl.ds(i * HEAD + lead, HEAD)] = q


def q_proj(h, w_qkv, b, cos, sin, width, block=512):
    rows, d = h.shape
    far = MOVED * HEAD
    return pl.pallas_call(
        q_kernel,
        grid=(width // block,),
        in_specs=[
            pl.BlockSpec((rows, d), lambda i: (0, 0)),
            pl.BlockSpec((d, block), lambda i: (0, i)),
            pl.BlockSpec((1, block), lambda i: (0, i)),
            pl.BlockSpec((rows, HEAD), lambda i: (0, 0)),
            pl.BlockSpec((rows, HEAD), lambda i: (0, 0)),
        ],
        out_specs=[pl.BlockSpec((rows, block), lambda i: (0, i)), pl.BlockSpec((rows, far), lambda i: (0, 0))],
        out_shape=[jax.ShapeDtypeStruct((rows, width), BF), jax.ShapeDtypeStruct((rows, far), BF)],
        compiler_params=pltpu.CompilerParams(dimension_semantics=("arbitrary",), vmem_limit_bytes=Q_VMEM),
        cost_estimate=pl.CostEstimate(flops=2 * rows * d * width, bytes_accessed=2 * d * width, transcendentals=0),
        name="q_proj",
    )(h, w_qkv, b, cos, sin)


HEADS = 16
MOVED = 3


def given(cp):
    return jnp.where(cp == 3, MOVED, jnp.where(cp == 2, 1, 0))


def taken(cp):
    return given(3 - cp)


STRIP = 256
CHUNK = 256


def attn_kernel(cp_ref, *refs, old, slots, first, far, far_first, backs):
    refs = list(refs)
    take = lambda n: [refs.pop(0) for _ in range(n)]
    far_q = take(2 if far else 0)
    own_q = take(2 if slots else 0)
    k_ref, vt_ref = take(2)
    back_refs = take(backs)
    far_outs = take(1 if far else 0)
    own_outs = take(1 if slots else 0)
    s_ref, p_ref, acc_ref, mx_ref, m_ref, l_ref, al_ref = take(7)
    slot = pl.program_id(0)
    if far and slots:
        q_ref, qn_ref = take(2)
        for at, ref, pair in ((slot, q_ref, (far_q[0], own_q[0])), (slot + 1, qn_ref, (far_q[1], own_q[1]))):
            for is_far, source in ((at < far, pair[0]), (at >= far, pair[1])):
                @pl.when(is_far)
                def _(ref=ref, source=source):
                    ref[...] = source[...]
    else:
        q_ref, qn_ref = far_q or own_q

    rows = q_ref.shape[0]
    strips = rows // STRIP
    chunks = rows // CHUNK
    cp = cp_ref[0]

    def owner_of(slot):
        other = jnp.where(far_first + slot < taken(cp), 3 - cp, -1)
        mine = jnp.where(first + slot - far < HEADS - given(cp), cp, -1)
        return jnp.where(slot < far, other, mine)

    owner = owner_of(slot)
    fresh = (slot == 0) | (owner_of(slot - 1) < 0)

    def scores(qr, base, u, w):
        k = k_ref[pl.ds(base + u * CHUNK, CHUNK), :]
        return lax.dot_general(k, qr[pl.ds(w * STRIP, STRIP), :], (((1,), (1,)), ((), ())), preferred_element_type=F32)

    def col_max(s):
        return s.reshape(CHUNK // 8, 8, STRIP).max(axis=0)

    def triangle(s):
        key = lax.broadcasted_iota(jnp.int32, s.shape, 0)
        query = lax.broadcasted_iota(jnp.int32, s.shape, 1)
        return jnp.where(key <= query, s, NEG)

    def product(base, u, w):
        at = base // HEAD + u * (CHUNK // HEAD)
        vt = jnp.concatenate([vt_ref[at + i] for i in range(CHUNK // HEAD)], axis=1)
        p = jnp.concatenate([p_ref[w * (STRIP // HEAD) + i, pl.ds(u * CHUNK, CHUNK), :] for i in range(STRIP // HEAD)], axis=1)
        return jnp.dot(vt, p, preferred_element_type=F32)

    def stage(ex=None, pv=None, qk=None, diagonal=False):
        for w in range(strips):
            ne = ex[w] if ex else 0
            np_ = pv[1][w] if pv else 0
            nq = qk[2][w] if qk else 0
            cs = pl.ds(w * STRIP, STRIP)
            total = None
            top = None
            if ne:
                m_old = m_ref[0:1, cs]
                m_new = jnp.maximum(m_old, mx_ref[:, cs].max(axis=0, keepdims=True))
                alpha = jnp.exp2((m_old - m_new) * SCALE2)
                l8 = l_ref[:, cs] * alpha
            for u in range(chunks):
                ks = pl.ds(u * CHUNK, CHUNK)
                if u < np_:
                    x = product(pv[0], u, w)
                    total = x if total is None else total + x
                if u < ne:
                    e = jnp.exp2((s_ref[ks, cs] - m_new) * SCALE2)
                    l8 = l8 + e.reshape(CHUNK // 8, 8, STRIP).sum(axis=0)
                    e = e.astype(BF)
                    for i in range(STRIP // HEAD):
                        p_ref[w * (STRIP // HEAD) + i, ks, :] = e[:, i * HEAD:(i + 1) * HEAD]
                if u < nq:
                    s = scores(qk[0], qk[1], u, w)
                    if diagonal and u == nq - 1:
                        s = triangle(s)
                    s_ref[ks, cs] = s
                    x = col_max(s)
                    top = x if top is None else jnp.maximum(top, x)
            if np_:
                acc_ref[:, cs] = acc_ref[:, cs] * al_ref[0:1, cs] + total
            if ne:
                m_ref[:, cs] = jnp.broadcast_to(m_new, (8, STRIP))
                al_ref[:, cs] = jnp.broadcast_to(alpha, (8, STRIP))
                l_ref[:, cs] = l8
            if nq:
                mx_ref[:, cs] = top

    full = [chunks] * strips
    upper = [w + 1 for w in range(strips)]

    @pl.when(fresh & (owner >= 0))
    def _():
        def strip(w, carry):
            cs = pl.ds(pl.multiple_of(w * STRIP, STRIP), STRIP)
            top = None
            for u in range(chunks):
                ks = pl.ds(u * CHUNK, CHUNK)
                s = lax.dot_general(k_ref[ks, :], q_ref[cs, :], (((1,), (1,)), ((), ())), preferred_element_type=F32)
                s_ref[ks, cs] = s
                top = col_max(s) if top is None else jnp.maximum(top, col_max(s))
            mx_ref[:, cs] = top
            return carry

        lax.fori_loop(0, strips, strip, 0)
        acc_ref[...] = jnp.zeros_like(acc_ref)

    @pl.when(owner >= 0)
    def _():
        own = pl.multiple_of(old + rows * owner, rows)
        m_ref[...] = jnp.full_like(m_ref, NEG)
        l_ref[...] = jnp.zeros_like(l_ref)
        stage(full, None, (q_ref, rows, full))

        def body(j, carry):
            before = pl.multiple_of((j - 1) * rows, rows)
            after = pl.multiple_of((j + 1) * rows, rows)
            stage(full, (before, full), (q_ref, after, full))
            return carry

        lax.fori_loop(1, own // rows - 1, body, 0)
        stage(full, (pl.multiple_of(own - 2 * rows, rows), full), (q_ref, own, upper), diagonal=True)
        stage(upper, (pl.multiple_of(own - rows, rows), full), (qn_ref, 0, full))
        stage(pv=(own, upper))
        outs = []
        for w in range(strips):
            cs = pl.ds(w * STRIP, STRIP)
            outs.append((acc_ref[:, cs] / l_ref[:, cs].sum(axis=0, keepdims=True)).astype(BF).T)

        def write(out):
            for w in range(strips):
                out[pl.ds(w * STRIP, STRIP), :] = outs[w]

        if far and slots:
            pl.when(slot < far)(functools.partial(write, far_outs[0]))
            pl.when(slot >= far)(functools.partial(write, own_outs[0]))
        else:
            write((far_outs + own_outs)[0])

    for i, back_ref in enumerate(back_refs):
        @pl.when((owner < 0) & ((slot == pl.num_programs(0) - 1) == (i == 0)))
        def _(back_ref=back_ref):
            own_outs[0][...] = back_ref[...]


def attention(cp, q, q_far, k_all, vt_all, *, slots=0, first=0, far=0, far_first=0, back=()):
    rows = k_all.shape[0] // 8
    keys = k_all.shape[0]
    row_block = lambda index: pl.BlockSpec((rows, HEAD), index)
    far_col = lambda s: MOVED - 1 - far_first - jnp.clip(s, 0, far - 1)
    own_col = lambda s: first + jnp.clip(s - far, 0, slots - 1)
    operands, in_specs, out_specs, out_shape = [], [], [], []
    for count, source, col, out_col in (
        (far, q_far, far_col, lambda s: far - 1 - jnp.clip(s, 0, far - 1)),
        (slots, q, own_col, lambda s: jnp.clip(s - far, 0, slots - 1)),
    ):
        if count:
            operands += [source, source]
            in_specs += [row_block(lambda s, c, col=col: (0, col(s))), row_block(lambda s, c, col=col: (0, col(s + 1)))]
            out_specs.append(row_block(lambda s, c, col=out_col: (0, col(s))))
            out_shape.append(jax.ShapeDtypeStruct((rows, count * HEAD), BF))
    operands += [k_all, vt_all, *back]
    in_specs += [
        pl.BlockSpec((keys, HEAD), lambda s, c: (0, 0)),
        pl.BlockSpec((keys // HEAD, HEAD, HEAD), lambda s, c: (0, 0, 0)),
    ]
    for i in range(len(back)):
        in_specs.append(row_block((lambda s, c: (0, 0)) if i == 0 else (lambda s, c: (0, jnp.clip(s - far - (slots - MOVED), 0, MOVED - 2)))))
    scratch = [
        pltpu.VMEM((rows, rows), F32),
        pltpu.VMEM((rows // HEAD, rows, HEAD), BF),
        pltpu.VMEM((HEAD, rows), F32),
    ] + [pltpu.VMEM((8, rows), F32)] * 4
    if far and slots:
        scratch += [pltpu.VMEM((rows, HEAD), BF)] * 2
    count = far + slots
    return pl.pallas_call(
        functools.partial(attn_kernel, old=keys // 2, slots=slots, first=first, far=far, far_first=far_first, backs=len(back)),
        grid_spec=pltpu.PrefetchScalarGridSpec(
            num_scalar_prefetch=1, grid=(count,), in_specs=in_specs, out_specs=out_specs, scratch_shapes=scratch
        ),
        out_shape=out_shape,
        compiler_params=pltpu.CompilerParams(dimension_semantics=("arbitrary",), vmem_limit_bytes=ATTN_VMEM),
        cost_estimate=pl.CostEstimate(flops=4 * rows * count * HEAD * keys, bytes_accessed=4 * rows * count * HEAD, transcendentals=0),
        name="attention",
    )(cp, *operands)


def gather_kernel(cp_ref, *refs):
    parts, (k_ref, vt_ref) = refs[:-2], refs[-2:]
    rows = k_ref.shape[0]
    for i, part in enumerate(parts):
        @pl.when(pl.program_id(0) == i)
        def _(part=part):
            k_ref[...] = part[pl.ds(0, rows), :]
            for b in range(rows // HEAD):
                vt_ref[b] = part[pl.ds(rows + b * HEAD, HEAD), :].T


def gather(cp, old, new):
    n = len(old)
    rows = old[0].shape[0] // 2
    place = lambda i, c: jnp.where(i < n, c[0] ^ i, n + lax.rem(c[0] + 2 * n - i, n))
    return pl.pallas_call(
        gather_kernel,
        grid_spec=pltpu.PrefetchScalarGridSpec(
            num_scalar_prefetch=1,
            grid=(2 * n,),
            in_specs=[pl.BlockSpec((2 * rows, HEAD), lambda i, c: (0, 0))] * (2 * n),
            out_specs=[
                pl.BlockSpec((rows, HEAD), lambda i, c: (place(i, c), 0)),
                pl.BlockSpec((rows // HEAD, HEAD, HEAD), lambda i, c: (place(i, c), 0, 0)),
            ],
        ),
        out_shape=[
            jax.ShapeDtypeStruct((2 * n * rows, HEAD), BF),
            jax.ShapeDtypeStruct((2 * n * rows // HEAD, HEAD, HEAD), BF),
        ],
        compiler_params=pltpu.CompilerParams(dimension_semantics=("arbitrary",), vmem_limit_bytes=ATTN_VMEM),
        cost_estimate=pl.CostEstimate(flops=2 ** 20, bytes_accessed=2 ** 23, transcendentals=0),
        name="gather",
    )(cp, *old, *new)


def own_kernel(x_ref, *rest):
    o_refs, w_ref, y_ref = rest[:-2], rest[-2], rest[-1]
    for r in range(x_ref.shape[0] // 256):
        rs = pl.ds(r * 256, 256)
        o = jnp.concatenate([o_ref[rs, :] for o_ref in o_refs], axis=1)
        y_ref[rs, :] = x_ref[rs, :].astype(F32) + jnp.dot(o, w_ref[...], preferred_element_type=F32)


def own_part(x, o_parts, w, block=512):
    rows, d = x.shape
    depth = w.shape[0]
    col = lambda i: (0, i)
    return pl.pallas_call(
        own_kernel,
        grid=(d // block,),
        in_specs=[pl.BlockSpec((rows, block), col)]
        + [pl.BlockSpec(o.shape, lambda i: (0, 0)) for o in o_parts]
        + [pl.BlockSpec((depth, block), col)],
        out_specs=pl.BlockSpec((rows, block), col),
        out_shape=jax.ShapeDtypeStruct((rows, d), F32),
        compiler_params=pltpu.CompilerParams(dimension_semantics=("arbitrary",), vmem_limit_bytes=OUT_VMEM),
        cost_estimate=pl.CostEstimate(flops=2 * rows * d * depth, bytes_accessed=6 * rows * d, transcendentals=0),
        name="own_part",
    )(x, *o_parts, w)


def other_kernel(cp_ref, y_ref, *rest, parts):
    o_refs, w_refs, out_ref, o_buf = rest[:parts], rest[parts:-2], rest[-2], rest[-1]

    @pl.when(pl.program_id(0) == 0)
    def _():
        at = 0
        for o_ref in o_refs:
            o_buf[:, pl.ds(at, o_ref.shape[1])] = o_ref[...]
            at += o_ref.shape[1]

    pieces = len(w_refs) // 4
    depth = sum(w_ref.shape[0] for w_ref in w_refs[:pieces])
    for r in range(y_ref.shape[0] // 256):
        rs = pl.ds(r * 256, 256)
        total = None
        for i in range(4):
            at = pl.multiple_of((cp_ref[0] ^ i) * depth, depth)
            w = jnp.concatenate([w_ref[...] for w_ref in w_refs[i * pieces:(i + 1) * pieces]], axis=0)
            x = jnp.dot(o_buf[rs, pl.ds(at, depth)], w, preferred_element_type=F32)
            total = x if total is None else total + x
        out_ref[rs, :] = (y_ref[rs, :] + total).astype(BF)


def other_part(cp, y, o_parts, w_parts, block=512):
    rows, d = y.shape
    col = lambda i, c: (0, i)
    depth = sum(w.shape[0] for w in w_parts)
    return pl.pallas_call(
        functools.partial(other_kernel, parts=len(o_parts)),
        grid_spec=pltpu.PrefetchScalarGridSpec(
            num_scalar_prefetch=1,
            grid=(d // block,),
            in_specs=[pl.BlockSpec((rows, block), col)]
            + [pl.BlockSpec(o.shape, lambda i, c: (0, 0)) for o in o_parts]
            + [pl.BlockSpec((w.shape[0], block), col) for w in w_parts],
            out_specs=pl.BlockSpec((rows, block), col),
            scratch_shapes=[pltpu.VMEM((rows, depth), BF)],
        ),
        out_shape=jax.ShapeDtypeStruct((rows, d), BF),
        compiler_params=pltpu.CompilerParams(dimension_semantics=("arbitrary",), vmem_limit_bytes=OTHER_VMEM),
        cost_estimate=pl.CostEstimate(flops=2 * rows * d * depth, bytes_accessed=6 * rows * d, transcendentals=0),
        name="other_part",
    )(cp, y, *o_parts, *w_parts)


SIZES = (5, 4, 3, 4)
PIECE_ROWS = (192, 320)
PIECES = len(PIECE_ROWS)


def after(a, *others):
    return lax.optimization_barrier((a, *others))[0]


def local_step(x, k_cache, v_cache, rope_table, norm_gain, w_qkv, b_qkv, w_out):
    rows = x.shape[0]
    n = lax.axis_size("cp")
    cp = lax.axis_index("cp")
    swap = [(0, 1), (1, 0)]
    width = w_out.shape[0]
    quarter = width // n
    where = cp.astype(jnp.int32)[None]
    around = lambda s: [(i, (i + s) % n) for i in range(n)]
    flip = lambda bits: [(i, i ^ bits) for i in range(n)]

    kv_cache = jnp.concatenate([k_cache[:, 0], v_cache[:, 0]], axis=0)
    old = [kv_cache, lax.ppermute(kv_cache, "cp", flip(1)), lax.ppermute(kv_cache, "cp", flip(2))]
    mine = lax.dynamic_slice_in_dim(w_out, cp * quarter, PIECE_ROWS[0], 0)
    w_peer = [lax.ppermute(mine, "tp", swap)]

    bias = b_qkv[None]
    h, kv_new, new_k, new_v, cos, sin, mine = norm_kv(where, x, norm_gain[None], w_qkv, bias, rope_table, w_out)
    w_peer.append(lax.ppermute(mine, "tp", swap))
    old.append(lax.ppermute(after(old[2], kv_new), "cp", flip(1)))
    kv_new = kv_new.reshape(2 * rows, HEAD)
    new = [kv_new] + [lax.ppermute(kv_new, "cp", around(s)) for s in range(1, n)]
    queries, q_far = q_proj(h, w_qkv, bias, cos, sin, width)
    q_far = lax.ppermute(q_far, "cp", [(3, 0), (2, 1)])
    w_peer[0] = after(w_peer[0], queries)

    k_all, vt_all = gather(where, old, new)
    attend = functools.partial(attention, where, k_all=k_all, vt_all=vt_all)

    o_own, o_other = [], []
    w_x, w_core, w_far = [None] * PIECES, [None] * PIECES, [None] * PIECES

    def heads(i, *previous, far=0, far_first=0, back=()):
        q = after(queries, *previous) if previous else queries
        outs = attend(q, q_far, slots=SIZES[i], first=sum(SIZES[:i]), far=far, far_first=far_first, back=back)
        o_own.append(outs[-1])
        o_other.append(lax.ppermute(outs[-1], "tp", swap))
        return outs

    def spread(i):
        w_x[i] = lax.ppermute(w_peer[i], "cp", flip(2))
        w_core[i] = lax.ppermute(w_peer[i], "cp", flip(1))

    def spread_on(i):
        w_far[i] = lax.ppermute(w_x[i], "cp", flip(1))

    spread(0)
    (part,) = heads(0)
    (far,) = attend(None, after(q_far, part), far=1)
    back0 = lax.ppermute(far, "cp", [(0, 3), (1, 2)])
    w_peer[1] = after(w_peer[1], far)
    spread(1)
    far, part = heads(1, far, far=MOVED - 1, far_first=1)
    back1 = lax.ppermute(far, "cp", [(0, 3)])
    (part,) = heads(2, part)
    (part,) = heads(3, part, back=(back0, back1))
    w_x = [after(w, part) for w in w_x]
    spread_on(0)
    spread_on(1)

    y = own_part(x, o_own, w_out)
    y = other_part(where, y, o_other, [*w_peer, *w_core, *w_x, *w_far])
    return y, new_k[:, None], new_v[:, None]


def solution(mesh):
    row_spec = P(("dp", "cp"), None)
    cache_spec = P(("dp", "cp"), "tp", None)
    return jax.shard_map(
        local_step,
        mesh=mesh,
        in_specs=(row_spec, cache_spec, cache_spec, row_spec, P(None), P(None, "tp"), P("tp"), P("tp", None)),
        out_specs=(row_spec, cache_spec, cache_spec),
        check_vma=False,
    )
```

```python
import functools
import math

import jax
import jax.numpy as jnp
from jax import lax
from jax.experimental import pallas as pl
from jax.experimental.pallas import tpu as pltpu
from jax.sharding import PartitionSpec as P


EPS = 1.5625e-07
NEG = -1e30
HEAD = 128
SCALE2 = HEAD ** -0.5 * math.log2(math.e)
F32 = jnp.float32
BF = jnp.bfloat16
ATTN_VMEM = 24 * 2 ** 20
NORM_VMEM = 36 * 2 ** 20
Q_VMEM = 36 * 2 ** 20
OUT_VMEM = 28 * 2 ** 20
OTHER_VMEM = 48 * 2 ** 20


def rotate(a, cos, sin):
    lane = lax.broadcasted_iota(jnp.int32, a.shape, 1)
    other = jnp.where(lane % 2 == 0, pltpu.roll(a, HEAD - 1, 1), pltpu.roll(a, 1, 1))
    return a * cos + other * sin


def norm_kv_kernel(cp_ref, x_ref, g_ref, w_ref, b_ref, table_ref, piece_ref, h_ref, kv_ref, k_ref, v_ref, cos_ref, sin_ref, copy_ref):
    copy_ref[...] = piece_ref[...]
    pairs = table_ref.shape[1] // 2
    lane = lax.broadcasted_iota(jnp.int32, (pairs, HEAD), 1)
    hit = lax.broadcasted_iota(jnp.int32, (pairs, HEAD), 0) == lane // 2
    spread = functools.partial(jnp.dot, precision=lax.Precision.HIGHEST, preferred_element_type=F32)
    stay = lax.broadcasted_iota(jnp.int32, (128, HEAD), 1) >= 2 * pairs
    for r in range(x_ref.shape[0] // 128):
        rs = pl.ds(r * 128, 128)
        table = table_ref[rs, :]
        cos = jnp.where(stay, 1.0, spread(table[:, :pairs], hit.astype(F32)))
        sin = spread(table[:, pairs:], jnp.where(hit, jnp.where(lane % 2 == 0, -1.0, 1.0), 0.0))
        cos_ref[rs, :] = cos
        sin_ref[rs, :] = sin
        x = x_ref[rs, :].astype(F32)
        inv = lax.rsqrt(jnp.mean(x * x, axis=-1, keepdims=True) + EPS)
        h = (x * inv * g_ref[...].astype(F32)).astype(BF)
        h_ref[rs, :] = h
        a = jnp.dot(h, w_ref[...], preferred_element_type=F32) + b_ref[...].astype(F32)
        k = rotate(a[:, :HEAD], cos, sin).astype(BF)
        v = a[:, HEAD:].astype(BF)
        k_ref[rs, :] = k
        v_ref[rs, :] = v
        kv_ref[0, rs, :] = k
        kv_ref[1, rs, :] = v


def norm_kv(cp, x, g, w_qkv, b, table, w_out, block=256):
    rows, d = x.shape
    steps = rows // block
    last = w_qkv.shape[1] // (2 * HEAD) - 1
    row = lambda i, c: (i, 0)
    skip, piece = PIECE_ROWS
    part = piece // steps
    quarter = skip + piece
    head_rows = pl.BlockSpec((block, HEAD), row)
    return pl.pallas_call(
        norm_kv_kernel,
        grid_spec=pltpu.PrefetchScalarGridSpec(
            num_scalar_prefetch=1,
            grid=(steps,),
            in_specs=[
                pl.BlockSpec((block, d), row),
                pl.BlockSpec((1, d), lambda i, c: (0, 0)),
                pl.BlockSpec((d, 2 * HEAD), lambda i, c: (0, last)),
                pl.BlockSpec((1, 2 * HEAD), lambda i, c: (0, last)),
                pl.BlockSpec((block, table.shape[1]), row),
                pl.BlockSpec((pl.Element(part), pl.Element(w_out.shape[1])), lambda i, c: (pl.multiple_of(c[0] * quarter + skip + i * part, 16), 0)),
            ],
            out_specs=[
                pl.BlockSpec((block, d), row),
                pl.BlockSpec((2, block, HEAD), lambda i, c: (0, i, 0)),
                head_rows,
                head_rows,
                head_rows,
                head_rows,
                pl.BlockSpec((part, w_out.shape[1]), row),
            ],
        ),
        out_shape=[
            jax.ShapeDtypeStruct((rows, d), BF),
            jax.ShapeDtypeStruct((2, rows, HEAD), BF),
            jax.ShapeDtypeStruct((rows, HEAD), BF),
            jax.ShapeDtypeStruct((rows, HEAD), BF),
            jax.ShapeDtypeStruct((rows, HEAD), F32),
            jax.ShapeDtypeStruct((rows, HEAD), F32),
            jax.ShapeDtypeStruct((piece, w_out.shape[1]), BF),
        ],
        compiler_params=pltpu.CompilerParams(dimension_semantics=("arbitrary",), vmem_limit_bytes=NORM_VMEM),
        cost_estimate=pl.CostEstimate(flops=2 * rows * d * 2 * HEAD, bytes_accessed=4 * rows * d, transcendentals=0),
        name="norm_kv",
    )(cp, x, g, w_qkv, b, table, w_out)


def q_kernel(h_ref, w_ref, b_ref, cos_ref, sin_ref, q_ref, far_ref):
    lead = far_ref.shape[1] - w_ref.shape[1]
    for r in range(h_ref.shape[0] // 128):
        rs = pl.ds(r * 128, 128)
        a = jnp.dot(h_ref[rs, :], w_ref[...], preferred_element_type=F32) + b_ref[...].astype(F32)
        for i in range(a.shape[1] // HEAD):
            at = slice(i * HEAD, (i + 1) * HEAD)
            q = rotate(a[:, at], cos_ref[rs, :], sin_ref[rs, :]).astype(BF)
            q_ref[rs, at] = q
            if i * HEAD + lead >= 0:
                far_ref[rs, pl.ds(i * HEAD + lead, HEAD)] = q


def q_proj(h, w_qkv, b, cos, sin, width, block=512):
    rows, d = h.shape
    far = MOVED * HEAD
    return pl.pallas_call(
        q_kernel,
        grid=(width // block,),
        in_specs=[
            pl.BlockSpec((rows, d), lambda i: (0, 0)),
            pl.BlockSpec((d, block), lambda i: (0, i)),
            pl.BlockSpec((1, block), lambda i: (0, i)),
            pl.BlockSpec((rows, HEAD), lambda i: (0, 0)),
            pl.BlockSpec((rows, HEAD), lambda i: (0, 0)),
        ],
        out_specs=[pl.BlockSpec((rows, block), lambda i: (0, i)), pl.BlockSpec((rows, far), lambda i: (0, 0))],
        out_shape=[jax.ShapeDtypeStruct((rows, width), BF), jax.ShapeDtypeStruct((rows, far), BF)],
        compiler_params=pltpu.CompilerParams(dimension_semantics=("arbitrary",), vmem_limit_bytes=Q_VMEM),
        cost_estimate=pl.CostEstimate(flops=2 * rows * d * width, bytes_accessed=2 * d * width, transcendentals=0),
        name="q_proj",
    )(h, w_qkv, b, cos, sin)


HEADS = 16
MOVED = 3


def given(cp):
    return jnp.where(cp == 3, MOVED, jnp.where(cp == 2, 1, 0))


def taken(cp):
    return given(3 - cp)


STRIP = 256
CHUNK = 256


def attn_kernel(cp_ref, *refs, old, slots, first, far, far_first, backs):
    refs = list(refs)
    take = lambda n: [refs.pop(0) for _ in range(n)]
    far_q = take(2 if far else 0)
    own_q = take(2 if slots else 0)
    k_ref, vt_ref = take(2)
    back_refs = take(backs)
    far_outs = take(1 if far else 0)
    own_outs = take(1 if slots else 0)
    s_ref, p_ref, acc_ref, mx_ref, m_ref, l_ref, al_ref = take(7)
    slot = pl.program_id(0)
    if far and slots:
        q_ref, qn_ref = take(2)
        for at, ref, pair in ((slot, q_ref, (far_q[0], own_q[0])), (slot + 1, qn_ref, (far_q[1], own_q[1]))):
            for is_far, source in ((at < far, pair[0]), (at >= far, pair[1])):
                @pl.when(is_far)
                def _(ref=ref, source=source):
                    ref[...] = source[...]
    else:
        q_ref, qn_ref = far_q or own_q

    rows = q_ref.shape[0]
    strips = rows // STRIP
    chunks = rows // CHUNK
    cp = cp_ref[0]

    def owner_of(slot):
        other = jnp.where(far_first + slot < taken(cp), 3 - cp, -1)
        mine = jnp.where(first + slot - far < HEADS - given(cp), cp, -1)
        return jnp.where(slot < far, other, mine)

    owner = owner_of(slot)
    fresh = (slot == 0) | (owner_of(slot - 1) < 0)

    def scores(qr, base, u, w):
        k = k_ref[pl.ds(base + u * CHUNK, CHUNK), :]
        return lax.dot_general(k, qr[pl.ds(w * STRIP, STRIP), :], (((1,), (1,)), ((), ())), preferred_element_type=F32)

    def col_max(s):
        return s.reshape(CHUNK // 8, 8, STRIP).max(axis=0)

    def triangle(s):
        key = lax.broadcasted_iota(jnp.int32, s.shape, 0)
        query = lax.broadcasted_iota(jnp.int32, s.shape, 1)
        return jnp.where(key <= query, s, NEG)

    def product(base, u, w):
        at = base // HEAD + u * (CHUNK // HEAD)
        vt = jnp.concatenate([vt_ref[at + i] for i in range(CHUNK // HEAD)], axis=1)
        p = jnp.concatenate([p_ref[w * (STRIP // HEAD) + i, pl.ds(u * CHUNK, CHUNK), :] for i in range(STRIP // HEAD)], axis=1)
        return jnp.dot(vt, p, preferred_element_type=F32)

    def stage(ex=None, pv=None, qk=None, diagonal=False):
        for w in range(strips):
            ne = ex[w] if ex else 0
            np_ = pv[1][w] if pv else 0
            nq = qk[2][w] if qk else 0
            cs = pl.ds(w * STRIP, STRIP)
            total = None
            top = None
            if ne:
                m_old = m_ref[0:1, cs]
                m_new = jnp.maximum(m_old, mx_ref[:, cs].max(axis=0, keepdims=True))
                alpha = jnp.exp2((m_old - m_new) * SCALE2)
                l8 = l_ref[:, cs] * alpha
            for u in range(chunks):
                ks = pl.ds(u * CHUNK, CHUNK)
                if u < np_:
                    x = product(pv[0], u, w)
                    total = x if total is None else total + x
                if u < ne:
                    e = jnp.exp2((s_ref[ks, cs] - m_new) * SCALE2)
                    l8 = l8 + e.reshape(CHUNK // 8, 8, STRIP).sum(axis=0)
                    e = e.astype(BF)
                    for i in range(STRIP // HEAD):
                        p_ref[w * (STRIP // HEAD) + i, ks, :] = e[:, i * HEAD:(i + 1) * HEAD]
                if u < nq:
                    s = scores(qk[0], qk[1], u, w)
                    if diagonal and u == nq - 1:
                        s = triangle(s)
                    s_ref[ks, cs] = s
                    x = col_max(s)
                    top = x if top is None else jnp.maximum(top, x)
            if np_:
                acc_ref[:, cs] = acc_ref[:, cs] * al_ref[0:1, cs] + total
            if ne:
                m_ref[:, cs] = jnp.broadcast_to(m_new, (8, STRIP))
                al_ref[:, cs] = jnp.broadcast_to(alpha, (8, STRIP))
                l_ref[:, cs] = l8
            if nq:
                mx_ref[:, cs] = top

    full = [chunks] * strips
    upper = [w + 1 for w in range(strips)]

    @pl.when(fresh & (owner >= 0))
    def _():
        def strip(w, carry):
            cs = pl.ds(pl.multiple_of(w * STRIP, STRIP), STRIP)
            top = None
            for u in range(chunks):
                ks = pl.ds(u * CHUNK, CHUNK)
                s = lax.dot_general(k_ref[ks, :], q_ref[cs, :], (((1,), (1,)), ((), ())), preferred_element_type=F32)
                s_ref[ks, cs] = s
                top = col_max(s) if top is None else jnp.maximum(top, col_max(s))
            mx_ref[:, cs] = top
            return carry

        lax.fori_loop(0, strips, strip, 0)
        acc_ref[...] = jnp.zeros_like(acc_ref)

    @pl.when(owner >= 0)
    def _():
        own = pl.multiple_of(old + rows * owner, rows)
        m_ref[...] = jnp.full_like(m_ref, NEG)
        l_ref[...] = jnp.zeros_like(l_ref)
        stage(full, None, (q_ref, rows, full))

        def body(j, carry):
            before = pl.multiple_of((j - 1) * rows, rows)
            after = pl.multiple_of((j + 1) * rows, rows)
            stage(full, (before, full), (q_ref, after, full))
            return carry

        lax.fori_loop(1, own // rows - 1, body, 0)
        stage(full, (pl.multiple_of(own - 2 * rows, rows), full), (q_ref, own, upper), diagonal=True)
        stage(upper, (pl.multiple_of(own - rows, rows), full), (qn_ref, 0, full))
        stage(pv=(own, upper))
        outs = []
        for w in range(strips):
            cs = pl.ds(w * STRIP, STRIP)
            outs.append((acc_ref[:, cs] / l_ref[:, cs].sum(axis=0, keepdims=True)).astype(BF).T)

        def write(out):
            for w in range(strips):
                out[pl.ds(w * STRIP, STRIP), :] = outs[w]

        if far and slots:
            pl.when(slot < far)(functools.partial(write, far_outs[0]))
            pl.when(slot >= far)(functools.partial(write, own_outs[0]))
        else:
            write((far_outs + own_outs)[0])

    for i, back_ref in enumerate(back_refs):
        @pl.when((owner < 0) & ((slot >= pl.num_programs(0) - 2) == (i == 0)))
        def _(back_ref=back_ref):
            own_outs[0][...] = back_ref[...]


def attention(cp, q, q_far, k_all, vt_all, *, slots=0, first=0, far=0, far_first=0, back=()):
    rows = k_all.shape[0] // 8
    keys = k_all.shape[0]
    row_block = lambda index: pl.BlockSpec((rows, HEAD), index)
    far_col = lambda s: MOVED - 1 - far_first - jnp.clip(s, 0, far - 1)
    own_col = lambda s: first + jnp.clip(s - far, 0, slots - 1)
    operands, in_specs, out_specs, out_shape = [], [], [], []
    for count, source, col, out_col in (
        (far, q_far, far_col, lambda s: far - 1 - jnp.clip(s, 0, far - 1)),
        (slots, q, own_col, lambda s: jnp.clip(s - far, 0, slots - 1)),
    ):
        if count:
            operands += [source, source]
            in_specs += [row_block(lambda s, c, col=col: (0, col(s))), row_block(lambda s, c, col=col: (0, col(s + 1)))]
            out_specs.append(row_block(lambda s, c, col=out_col: (0, col(s))))
            out_shape.append(jax.ShapeDtypeStruct((rows, count * HEAD), BF))
    operands += [k_all, vt_all, *back]
    in_specs += [
        pl.BlockSpec((keys, HEAD), lambda s, c: (0, 0)),
        pl.BlockSpec((keys // HEAD, HEAD, HEAD), lambda s, c: (0, 0, 0)),
    ]
    for i in range(len(back)):
        in_specs.append(row_block((lambda s, c: (0, jnp.clip(s - far - (slots - 2), 0, 1))) if i == 0 else (lambda s, c: (0, 0))))
    scratch = [
        pltpu.VMEM((rows, rows), F32),
        pltpu.VMEM((rows // HEAD, rows, HEAD), BF),
        pltpu.VMEM((HEAD, rows), F32),
    ] + [pltpu.VMEM((8, rows), F32)] * 4
    if far and slots:
        scratch += [pltpu.VMEM((rows, HEAD), BF)] * 2
    count = far + slots
    return pl.pallas_call(
        functools.partial(attn_kernel, old=keys // 2, slots=slots, first=first, far=far, far_first=far_first, backs=len(back)),
        grid_spec=pltpu.PrefetchScalarGridSpec(
            num_scalar_prefetch=1, grid=(count,), in_specs=in_specs, out_specs=out_specs, scratch_shapes=scratch
        ),
        out_shape=out_shape,
        compiler_params=pltpu.CompilerParams(dimension_semantics=("arbitrary",), vmem_limit_bytes=ATTN_VMEM),
        cost_estimate=pl.CostEstimate(flops=4 * rows * count * HEAD * keys, bytes_accessed=4 * rows * count * HEAD, transcendentals=0),
        name="attention",
    )(cp, *operands)


def gather_kernel(cp_ref, *refs):
    parts, (k_ref, vt_ref) = refs[:-2], refs[-2:]
    rows = k_ref.shape[0]
    for i, part in enumerate(parts):
        @pl.when(pl.program_id(0) == i)
        def _(part=part):
            k_ref[...] = part[pl.ds(0, rows), :]
            for b in range(rows // HEAD):
                vt_ref[b] = part[pl.ds(rows + b * HEAD, HEAD), :].T


def gather(cp, old, new):
    n = len(old)
    rows = old[0].shape[0] // 2
    place = lambda i, c: jnp.where(i < n, c[0] ^ i, n + lax.rem(c[0] + 2 * n - i, n))
    return pl.pallas_call(
        gather_kernel,
        grid_spec=pltpu.PrefetchScalarGridSpec(
            num_scalar_prefetch=1,
            grid=(2 * n,),
            in_specs=[pl.BlockSpec((2 * rows, HEAD), lambda i, c: (0, 0))] * (2 * n),
            out_specs=[
                pl.BlockSpec((rows, HEAD), lambda i, c: (place(i, c), 0)),
                pl.BlockSpec((rows // HEAD, HEAD, HEAD), lambda i, c: (place(i, c), 0, 0)),
            ],
        ),
        out_shape=[
            jax.ShapeDtypeStruct((2 * n * rows, HEAD), BF),
            jax.ShapeDtypeStruct((2 * n * rows // HEAD, HEAD, HEAD), BF),
        ],
        compiler_params=pltpu.CompilerParams(dimension_semantics=("arbitrary",), vmem_limit_bytes=ATTN_VMEM),
        cost_estimate=pl.CostEstimate(flops=2 ** 20, bytes_accessed=2 ** 23, transcendentals=0),
        name="gather",
    )(cp, *old, *new)


def own_kernel(x_ref, *rest):
    o_refs, w_ref, y_ref = rest[:-2], rest[-2], rest[-1]
    for r in range(x_ref.shape[0] // 256):
        rs = pl.ds(r * 256, 256)
        o = jnp.concatenate([o_ref[rs, :] for o_ref in o_refs], axis=1)
        y_ref[rs, :] = x_ref[rs, :].astype(F32) + jnp.dot(o, w_ref[...], preferred_element_type=F32)


def own_part(x, o_parts, w, block=512):
    rows, d = x.shape
    depth = w.shape[0]
    col = lambda i: (0, i)
    return pl.pallas_call(
        own_kernel,
        grid=(d // block,),
        in_specs=[pl.BlockSpec((rows, block), col)]
        + [pl.BlockSpec(o.shape, lambda i: (0, 0)) for o in o_parts]
        + [pl.BlockSpec((depth, block), col)],
        out_specs=pl.BlockSpec((rows, block), col),
        out_shape=jax.ShapeDtypeStruct((rows, d), F32),
        compiler_params=pltpu.CompilerParams(dimension_semantics=("arbitrary",), vmem_limit_bytes=OUT_VMEM),
        cost_estimate=pl.CostEstimate(flops=2 * rows * d * depth, bytes_accessed=6 * rows * d, transcendentals=0),
        name="own_part",
    )(x, *o_parts, w)


def other_kernel(cp_ref, y_ref, *rest, parts):
    o_refs, w_refs, out_ref, o_buf = rest[:parts], rest[parts:-2], rest[-2], rest[-1]

    @pl.when(pl.program_id(0) == 0)
    def _():
        at = 0
        for o_ref in o_refs:
            o_buf[:, pl.ds(at, o_ref.shape[1])] = o_ref[...]
            at += o_ref.shape[1]

    pieces = len(w_refs) // 4
    depth = sum(w_ref.shape[0] for w_ref in w_refs[:pieces])
    for r in range(y_ref.shape[0] // 256):
        rs = pl.ds(r * 256, 256)
        total = None
        for i in range(4):
            at = pl.multiple_of((cp_ref[0] ^ i) * depth, depth)
            w = jnp.concatenate([w_ref[...] for w_ref in w_refs[i * pieces:(i + 1) * pieces]], axis=0)
            x = jnp.dot(o_buf[rs, pl.ds(at, depth)], w, preferred_element_type=F32)
            total = x if total is None else total + x
        out_ref[rs, :] = (y_ref[rs, :] + total).astype(BF)


def other_part(cp, y, o_parts, w_parts, block=512):
    rows, d = y.shape
    col = lambda i, c: (0, i)
    depth = sum(w.shape[0] for w in w_parts)
    return pl.pallas_call(
        functools.partial(other_kernel, parts=len(o_parts)),
        grid_spec=pltpu.PrefetchScalarGridSpec(
            num_scalar_prefetch=1,
            grid=(d // block,),
            in_specs=[pl.BlockSpec((rows, block), col)]
            + [pl.BlockSpec(o.shape, lambda i, c: (0, 0)) for o in o_parts]
            + [pl.BlockSpec((w.shape[0], block), col) for w in w_parts],
            out_specs=pl.BlockSpec((rows, block), col),
            scratch_shapes=[pltpu.VMEM((rows, depth), BF)],
        ),
        out_shape=jax.ShapeDtypeStruct((rows, d), BF),
        compiler_params=pltpu.CompilerParams(dimension_semantics=("arbitrary",), vmem_limit_bytes=OTHER_VMEM),
        cost_estimate=pl.CostEstimate(flops=2 * rows * d * depth, bytes_accessed=6 * rows * d, transcendentals=0),
        name="other_part",
    )(cp, y, *o_parts, *w_parts)


SIZES = (6, 4, 2, 4)
PIECE_ROWS = (192, 320)
PIECES = len(PIECE_ROWS)


def after(a, *others):
    return lax.optimization_barrier((a, *others))[0]


def local_step(x, k_cache, v_cache, rope_table, norm_gain, w_qkv, b_qkv, w_out):
    rows = x.shape[0]
    n = lax.axis_size("cp")
    cp = lax.axis_index("cp")
    swap = [(0, 1), (1, 0)]
    width = w_out.shape[0]
    quarter = width // n
    where = cp.astype(jnp.int32)[None]
    around = lambda s: [(i, (i + s) % n) for i in range(n)]
    flip = lambda bits: [(i, i ^ bits) for i in range(n)]

    kv_cache = jnp.concatenate([k_cache[:, 0], v_cache[:, 0]], axis=0)
    old = [kv_cache, lax.ppermute(kv_cache, "cp", flip(1)), lax.ppermute(kv_cache, "cp", flip(2))]
    mine = lax.dynamic_slice_in_dim(w_out, cp * quarter, PIECE_ROWS[0], 0)
    w_peer = [lax.ppermute(mine, "tp", swap)]

    bias = b_qkv[None]
    h, kv_new, new_k, new_v, cos, sin, mine = norm_kv(where, x, norm_gain[None], w_qkv, bias, rope_table, w_out)
    w_peer.append(lax.ppermute(mine, "tp", swap))
    old.append(lax.ppermute(after(old[2], kv_new), "cp", flip(1)))
    kv_new = kv_new.reshape(2 * rows, HEAD)
    new = [kv_new] + [lax.ppermute(kv_new, "cp", around(s)) for s in range(1, n)]
    queries, q_far = q_proj(h, w_qkv, bias, cos, sin, width)
    q_far = lax.ppermute(q_far, "cp", [(3, 0), (2, 1)])
    w_peer[0] = after(w_peer[0], queries)

    k_all, vt_all = gather(where, old, new)
    attend = functools.partial(attention, where, k_all=k_all, vt_all=vt_all)

    o_own, o_other = [], []
    w_x, w_core, w_far = [None] * PIECES, [None] * PIECES, [None] * PIECES

    def heads(i, *previous, far=0, far_first=0, back=()):
        q = after(queries, *previous) if previous else queries
        outs = attend(q, q_far, slots=SIZES[i], first=sum(SIZES[:i]), far=far, far_first=far_first, back=back)
        o_own.append(outs[-1])
        o_other.append(lax.ppermute(outs[-1], "tp", swap))
        return outs

    def spread(i):
        w_x[i] = lax.ppermute(w_peer[i], "cp", flip(2))
        w_core[i] = lax.ppermute(w_peer[i], "cp", flip(1))

    def spread_on(i):
        w_far[i] = lax.ppermute(w_x[i], "cp", flip(1))

    spread(0)
    (part,) = heads(0)
    (far,) = attend(None, after(q_far, part), far=2)
    back0 = lax.ppermute(far, "cp", [(0, 3), (1, 2)])
    w_peer[1] = after(w_peer[1], far)
    spread(1)
    far, part = heads(1, far, far=1, far_first=2)
    back1 = lax.ppermute(far, "cp", [(0, 3)])
    (part,) = heads(2, part)
    (part,) = heads(3, part, back=(back0, back1))
    w_x = [after(w, part) for w in w_x]
    spread_on(0)
    spread_on(1)

    y = own_part(x, o_own, w_out)
    y = other_part(where, y, o_other, [*w_peer, *w_core, *w_x, *w_far])
    return y, new_k[:, None], new_v[:, None]


def solution(mesh):
    row_spec = P(("dp", "cp"), None)
    cache_spec = P(("dp", "cp"), "tp", None)
    return jax.shard_map(
        local_step,
        mesh=mesh,
        in_specs=(row_spec, cache_spec, cache_spec, row_spec, P(None), P(None, "tp"), P("tp"), P("tp", None)),
        out_specs=(row_spec, cache_spec, cache_spec),
        check_vma=False,
    )
```
